8 devices in a mesh: ens: 2 (over z, y), feat: 4 (over x, core).
Axes of the slice: x: 2, y: 2, z: 1, core: 2. Of those that a mesh axis runs over, the one named last changes fastest.
Arguments:
- particles: float32 [768, 16384], P('ens', 'feat'), parts along dimension 0
- prec_diag: float32 [32768], P(('ens', 'feat')), parts along dimension 0
- low_factor: bfloat16 [32768, 16], P(('ens', 'feat')), parts along dimension 0
- prior_mean: float32 [32768], P(('ens', 'feat')), parts along dimension 0
- data_mat: bfloat16 [1536, 16384], P('ens', 'feat'), parts along dimension 0
- labels: int32 [1536], P('ens'), parts along dimension 0
Outputs:
- output: float32 [768, 16384], P('ens', 'feat'), parts along dimension 0
There are 2 independent parts. The reference program is written for one: setup_inputs(seed, part) draws one part's arguments, and reference() takes and returns one part's arrays. A program takes and returns all parts, laid end to end along the dimension named above; each array names one.
All inputs are finite; a program needn't handle non-finite values.
Results may differ from the reference program's by a relative error of at most 0.001.
Values are sent between devices in bfloat16 or wider.
A program may use at most 1 GiB of HBM per device.

```python
import math
import jax
import jax.numpy as jnp

FEAT_DIM = 16384
LOW_RANK = 16
PARTICLES = 384
DATA_ROWS = 768
NUM_STEPS = 3


def setup_inputs(seed: int = 0, part: int = 0) -> dict:
    base_key = jax.random.fold_in(jax.random.key(seed), part)
    sub_keys = jax.random.split(base_key, 8)
    common = jax.random.normal(sub_keys[0], (1, FEAT_DIM), jnp.float32)
    spread = jax.random.uniform(sub_keys[1], (PARTICLES, 1), jnp.float32, 0.5, 1.5)
    noise_mat = jax.random.normal(sub_keys[2], (PARTICLES, FEAT_DIM), jnp.float32)
    particles = common + spread * noise_mat
    prec_diag = jnp.exp(jax.random.uniform(sub_keys[3], (FEAT_DIM,), jnp.float32, -1.0, 1.0)) / FEAT_DIM
    u_scale = 1.1 * (FEAT_DIM * math.sqrt(LOW_RANK * FEAT_DIM)) ** -0.5
    low_factor = (jax.random.normal(sub_keys[4], (FEAT_DIM, LOW_RANK), jnp.float32) * u_scale).astype(jnp.bfloat16)
    prior_mean = 0.5 * jax.random.normal(sub_keys[5], (FEAT_DIM,), jnp.float32)
    data_scale = 1.5 / math.sqrt(FEAT_DIM)
    data_mat = (jax.random.normal(sub_keys[6], (DATA_ROWS, FEAT_DIM), jnp.float32) * data_scale).astype(jnp.bfloat16)
    labels = jax.random.randint(sub_keys[7], (DATA_ROWS,), 0, 2, jnp.int32)
    return {"particles": particles, "prec_diag": prec_diag, "low_factor": low_factor,
            "prior_mean": prior_mean, "data_mat": data_mat, "labels": labels}


def reference(particles, prec_diag, low_factor, prior_mean, data_mat, labels):
    band_width = 2.0 * FEAT_DIM
    step_size = FEAT_DIM / 4.0
    lik_weight = 2.0 / math.sqrt(DATA_ROWS * FEAT_DIM)
    targets = labels.astype(jnp.float32)[None, :]
    state = particles
    for step_idx in range(NUM_STEPS):
        part_bf = state.astype(jnp.bfloat16)
        centred = state - prior_mean
        projected = jnp.dot(centred.astype(jnp.bfloat16), low_factor, preferred_element_type=jnp.float32)
        gram_mat = jnp.dot(part_bf, part_bf.T, preferred_element_type=jnp.float32)
        sq_norm = jnp.diagonal(gram_mat)
        sq_dist = jnp.maximum(sq_norm[:, None] + sq_norm[None, :] - 2.0 * gram_mat, 0.0)
        kernel = jnp.exp(-sq_dist / band_width)
        logits = jnp.dot(part_bf, data_mat.T, preferred_element_type=jnp.float32)
        residual = targets - jax.nn.sigmoid(logits)
        low_rank = jnp.dot(projected.astype(jnp.bfloat16), low_factor.T, preferred_element_type=jnp.float32)
        lik_term = jnp.dot(residual.astype(jnp.bfloat16), data_mat, preferred_element_type=jnp.float32)
        log_grad = lik_weight * lik_term - centred * prec_diag - low_rank
        kern_bf = kernel.astype(jnp.bfloat16)
        driving = jnp.dot(kern_bf, log_grad.astype(jnp.bfloat16), preferred_element_type=jnp.float32)
        pulled = jnp.dot(kern_bf, part_bf, preferred_element_type=jnp.float32)
        row_sum = jnp.sum(kernel, axis=1, keepdims=True)
        update_dir = (driving + (2.0 / band_width) * (row_sum * state - pulled)) / PARTICLES
        state = state + step_size * update_dir
    return state
```

```python
import functools
import math

import jax
import jax.numpy as jnp
from jax import lax
from jax.experimental import pallas as pl
from jax.experimental.pallas import tpu as pltpu
from jax.sharding import PartitionSpec as P

NUM_STEPS = 3
DIMS_NT = (((1,), (1,)), ((), ()))
MESH = pl.DeviceIdType.MESH
F32 = jnp.float32
BF16 = jnp.bfloat16

NP = 384
MD = 768
CH = 256
NC = MD // CH
OWN = NP // 4
PH = 328
BF = 512

D2D_Z, ICI_Z, ICI_R, D2D_R, D2D_F = 0, NC, 2 * NC, 3 * NC, 4 * NC
D2D_P = 5 * NC
ICI_P, D2D_PG, D2D_Q, ICI_Q, D2D_QG = (D2D_P + i for i in range(1, 6))
N_SEM = D2D_P + 6


def kernel(beta, c1, c2, inv_h, th_hbm, lam, mu, u, a_hbm, y, out_hbm,
           th, a, tb, base, zp, zr1, zr2, rb, pp, pr1, pr2, pf, qp, qr1, qr2, qf,
           kb, krow, qb, ss, rs, ls):
    dim = th.shape[1]
    nb = dim // BF
    me = lax.axis_index("feat")
    x, core = lax.div(me, 2), lax.rem(me, 2)
    ox, oc = 1 - x, 1 - core
    partner, cross = x * 2 + oc, ox * 2 + core

    def remote(src, dst, slot, dev):
        return pltpu.make_async_remote_copy(
            src_ref=src, dst_ref=dst, send_sem=ss.at[slot], recv_sem=rs.at[slot],
            device_id={"feat": dev}, device_id_type=MESH)

    def cols(b):
        return pl.ds(pl.multiple_of(b * BF, BF), BF)

    def th_load(b):
        return pltpu.make_async_copy(th_hbm.at[:, cols(b)], th.at[:, cols(b)], ls.at[b])

    def a_load(c):
        return pltpu.make_async_copy(a_hbm.at[pl.ds(c * CH, CH)], a.at[pl.ds(c * CH, CH)], ls.at[nb + c])

    def out_store(b):
        return pltpu.make_async_copy(th.at[:, cols(b)], out_hbm.at[:, cols(b)], ls.at[nb + NC + b])

    for b in range(nb):
        th_load(b).start()
    for c in range(NC):
        a_load(c).start()

    barrier = pltpu.get_barrier_semaphore()
    for dev in (partner, cross):
        pl.semaphore_signal(barrier, inc=1, device_id={"feat": dev}, device_id_type=MESH)
    pl.semaphore_wait(barrier, 2)

    def conv(b, carry):
        th_load(b).wait()
        tb[:, cols(b)] = th[:, cols(b)].astype(BF16)
        return carry

    lax.fori_loop(0, nb, conv, 0)
    for c in range(NC):
        a_load(c).wait()

    rows_i = lax.broadcasted_iota(jnp.int32, (128, 128), 0)
    cols_i = lax.broadcasted_iota(jnp.int32, (128, 128), 1)

    def step_body(step, carry):
        d2d_z = [remote(zp.at[c, oc], zr1.at[c], D2D_Z + c, partner) for c in range(NC)]
        ici_z = [remote(zp.at[c, core, ox], zr2.at[c], ICI_Z + c, cross) for c in range(NC)]
        ici_r = [remote(rb.at[c, core, x], rb.at[c, core, x], ICI_R + c, cross) for c in range(NC)]
        d2d_r = [remote(rb.at[c, core, x], rb.at[c, core, x], D2D_R + c, partner) for c in range(NC)]
        d2d_f = [remote(rb.at[c, core, ox], rb.at[c, core, ox], D2D_F + c, partner) for c in range(NC)]
        d2d_p = remote(pp.at[oc], pr1, D2D_P, partner)
        ici_p = remote(pp.at[core], pr2, ICI_P, cross)
        d2d_pg = remote(pf.at[core], pf.at[core], D2D_PG, partner)
        d2d_q = remote(qp.at[oc], qr1, D2D_Q, partner)
        ici_q = remote(qp.at[core], qr2, ICI_Q, cross)
        d2d_qg = remote(qf.at[core], qf.at[core], D2D_QG, partner)

        def z_dot(c):
            z = lax.dot_general(tb[...], a[pl.ds(c * CH, CH), :], DIMS_NT, preferred_element_type=F32)
            zp[c] = z.reshape(2, 2, OWN, CH)
            d2d_z[c].start()

        def z_chip(c):
            d2d_z[c].wait_recv()
            zp[c, core] = zp[c, core] + zr1[c].reshape(2, OWN, CH)
            ici_z[c].start()

        def r_own(c):
            ici_z[c].wait_recv()
            z = zp[c, core, x] + zr2[c]
            r = y[:, pl.ds(c * CH, CH)].astype(F32) - jax.nn.sigmoid(z)
            rb[c, core, x] = r.astype(BF16)
            ici_r[c].start()
            d2d_r[c].start()

        def r_forward(c):
            ici_r[c].wait_recv()
            d2d_f[c].start()

        def r_all(c):
            d2d_r[c].wait_recv()
            d2d_f[c].wait_recv()

        z_dot(0)
        ga = lax.dot_general(tb[...], tb[0:256, :], DIMS_NT, preferred_element_type=F32)
        z_chip(0)
        d2 = lax.dot_general(tb[256:384, :], tb[256:384, :], DIMS_NT, preferred_element_type=F32)
        d0, d1 = ga[0:128, 0:128], ga[128:256, 128:256]

        def diag_row(d):
            return jnp.sum(jnp.where(rows_i == cols_i, d, 0.0), axis=0, keepdims=True)

        rid = lax.broadcasted_iota(jnp.int32, (16, 128), 0)
        diag = jnp.where(rid == 0, diag_row(d0), jnp.where(rid == 1, diag_row(d1), diag_row(d2)))
        packed = jnp.concatenate(
            [ga[128:256, 0:128], ga[256:384, 0:128], ga[256:384, 128:256],
             jnp.where(rows_i >= cols_i, d0, d1), d2, diag], axis=0)
        pp[0] = packed[0:PH]
        pp[1] = packed[PH:2 * PH]
        d2d_p.start()

        z_dot(1)
        d2d_p.wait_recv()
        pp[core] = pp[core] + pr1[...]
        ici_p.start()

        def q_block(b, acc):
            xb = (th[:, cols(b)] - mu[:, cols(b)]).astype(BF16)
            return acc + jnp.dot(xb, u[pl.ds(pl.multiple_of(b * BF, BF), BF), :], preferred_element_type=F32)

        q = lax.fori_loop(0, nb, q_block, jnp.zeros((NP, 16), F32))
        qp[...] = q.T.reshape(2, 8, NP)
        d2d_q.start()

        z_dot(2)
        d2d_q.wait_recv()
        qp[core] = qp[core] + qr1[...]
        ici_q.start()
        z_chip(1)
        z_chip(2)
        r_own(0)

        ici_p.wait_recv()
        pf[core] = pp[core] + pr2[...]
        d2d_pg.start()
        ici_q.wait_recv()
        qf[core] = qp[core] + qr2[...]
        d2d_qg.start()
        d2d_pg.wait_recv()

        full = pf[...].reshape(2 * PH, 128)
        n_row = [full[640 + i:641 + i, :] for i in range(3)]
        n_col = [jnp.sum(jnp.where(rows_i == cols_i, n, 0.0), axis=1, keepdims=True) for n in n_row]

        def kern(ni, nj, g):
            return jnp.exp(-(jnp.maximum(ni + nj - 2.0 * g, 0.0) * inv_h))

        k10 = kern(n_col[1], n_row[0], full[0:128])
        k20 = kern(n_col[2], n_row[0], full[128:256])
        k21 = kern(n_col[2], n_row[1], full[256:384])
        low = rows_i >= cols_i
        kmix = kern(jnp.where(low, n_col[0], n_col[1]), jnp.where(low, n_row[0], n_row[1]), full[384:512])
        k22 = kern(n_col[2], n_row[2], full[512:640])
        kmix_t = kmix.T
        k00 = jnp.where(low, kmix, kmix_t)
        k11 = jnp.where(rows_i < cols_i, kmix, jnp.where(rows_i > cols_i, kmix_t, 1.0))
        kmat = [[k00, k10.T, k20.T], [k10, k11, k21.T], [k20, k21, k22]]
        for i in range(3):
            for j in range(3):
                kb[128 * i:128 * (i + 1), 128 * j:128 * (j + 1)] = kmat[i][j].astype(BF16)
            k_sum = jnp.sum(kmat[i][0] + kmat[i][1] + kmat[i][2], axis=1, keepdims=True)
            krow[128 * i:128 * (i + 1), :] = jnp.broadcast_to(k_sum, (128, 128))

        d2d_qg.wait_recv()
        qb[...] = qf[...].reshape(16, NP).T.astype(BF16)

        r_own(1)

        def base_block(b, carry):
            t = th[:, cols(b)]
            low_rank = lax.dot_general(qb[...], u[pl.ds(pl.multiple_of(b * BF, BF), BF), :], DIMS_NT,
                                       preferred_element_type=F32)
            base[:, cols(b)] = -((t - mu[:, cols(b)]) * lam[:, cols(b)]) - low_rank
            pulled = jnp.dot(kb[...], tb[:, cols(b)], preferred_element_type=F32)
            th[:, cols(b)] = t + c1 * (krow[:, 0:1] * t - pulled)
            return carry

        lax.fori_loop(0, nb // 2, base_block, 0)
        r_own(2)
        lax.fori_loop(nb // 2, nb, base_block, 0)

        def ra_chunk(c):
            def ra_block(b, carry):
                ra = jnp.dot(rb[c].reshape(NP, CH), a[pl.ds(c * CH, CH), cols(b)], preferred_element_type=F32)
                base[:, cols(b)] = base[:, cols(b)] + beta * ra
                return carry
            lax.fori_loop(0, nb, ra_block, 0)

        r_forward(0)
        r_forward(1)
        r_all(0)
        ra_chunk(0)
        r_forward(2)
        r_all(1)
        ra_chunk(1)
        r_all(2)

        def final_block(b, carry):
            c = NC - 1
            ra = jnp.dot(rb[c].reshape(NP, CH), a[pl.ds(c * CH, CH), cols(b)], preferred_element_type=F32)
            s = (base[:, cols(b)] + beta * ra).astype(BF16)
            t = th[:, cols(b)] + c2 * jnp.dot(kb[...], s, preferred_element_type=F32)
            th[:, cols(b)] = t
            tb[:, cols(b)] = t.astype(BF16)

            @pl.when(step == NUM_STEPS - 1)
            def _():
                out_store(b).start()
            return carry

        lax.fori_loop(0, nb, final_block, 0)

        for cp in d2d_z + ici_z + ici_r + d2d_r + d2d_f + [d2d_p, ici_p, d2d_pg, d2d_q, ici_q, d2d_qg]:
            cp.wait_send()
        return carry

    lax.fori_loop(0, NUM_STEPS, step_body, 0)
    for b in range(nb):
        out_store(b).wait()


def solution(mesh):
    feat_size = mesh.shape["feat"]

    def local_run(particles, prec_diag, low_factor, prior_mean, data_mat, labels):
        n_part, dim_local = particles.shape
        dim_full = dim_local * feat_size
        m_rows = data_mat.shape[0]
        band_width = 2.0 * dim_full
        step_size = dim_full / 4.0
        beta = 2.0 / math.sqrt(m_rows * dim_full)
        c1 = step_size * (2.0 / band_width) / n_part
        c2 = step_size / n_part
        nb = dim_local // BF
        vm = pltpu.VMEM
        scratch = [
            vm((NP, dim_local), F32),
            vm((MD, dim_local), BF16),
            vm((NP, dim_local), BF16),
            vm((NP, dim_local), F32),
            vm((NC, 2, 2, OWN, CH), F32),
            vm((NC, 2, OWN, CH), F32),
            vm((NC, OWN, CH), F32),
            vm((NC, 2, 2, OWN, CH), BF16),
            vm((2, PH, 128), F32),
            vm((PH, 128), F32),
            vm((PH, 128), F32),
            vm((2, PH, 128), F32),
            vm((2, 8, NP), F32),
            vm((8, NP), F32),
            vm((8, NP), F32),
            vm((2, 8, NP), F32),
            vm((NP, NP), BF16),
            vm((NP, 128), F32),
            vm((NP, 16), BF16),
            pltpu.SemaphoreType.DMA((N_SEM,)),
            pltpu.SemaphoreType.DMA((N_SEM,)),
            pltpu.SemaphoreType.DMA((2 * nb + NC,)),
        ]
        anyspec = pl.BlockSpec(memory_space=pl.ANY)
        vspec = pl.BlockSpec(memory_space=pltpu.VMEM)
        return pl.pallas_call(
            functools.partial(kernel, beta, c1, c2, 1.0 / band_width),
            out_shape=jax.ShapeDtypeStruct((n_part, dim_local), F32),
            in_specs=[anyspec, vspec, vspec, vspec, anyspec, vspec],
            out_specs=anyspec,
            scratch_shapes=scratch,
            compiler_params=pltpu.CompilerParams(
                collective_id=0, has_side_effects=True, vmem_limit_bytes=60 * 1024 * 1024),
            name="svgd",
        )(particles, prec_diag.reshape(1, dim_local), prior_mean.reshape(1, dim_local), low_factor,
          data_mat, labels.reshape(1, m_rows))

    return jax.shard_map(
        local_run,
        mesh=mesh,
        in_specs=(P("ens", "feat"), P(("ens", "feat")), P(("ens", "feat"), None),
                  P(("ens", "feat")), P("ens", "feat"), P("ens")),
        out_specs=P("ens", "feat"),
        check_vma=False,
    )
```

```python
import functools
import math

import jax
import jax.numpy as jnp
from jax import lax
from jax.experimental import pallas as pl
from jax.experimental.pallas import tpu as pltpu
from jax.sharding import PartitionSpec as P

NUM_STEPS = 3
DIMS_NT = (((1,), (1,)), ((), ()))
MESH = pl.DeviceIdType.MESH
F32 = jnp.float32
BF16 = jnp.bfloat16

NP = 384
MD = 768
CH = 256
NC = MD // CH
OWN = NP // 4
QR = 144
BL = 512
BQ = 4096
BB = 4096
BK = 4096
BR = 4096
BU = 4096

D2D_Z, ICI_Z, ICI_R, D2D_R, D2D_F = 0, NC, 2 * NC, 3 * NC, 4 * NC
(D2D_P, ICI_P, ICI_K, D2D_K, FWD_K, ICI_S, D2D_S, FWD_S,
 D2D_Q, ICI_Q, D2D_QG) = range(5 * NC, 5 * NC + 11)
N_SEM = 5 * NC + 11


def kernel(beta, c1, c2, two_h, inv_h, th_hbm, lam_hbm, mu_hbm, u_hbm, a_hbm, y_hbm, th,
           lam, mu, u, y, a, at, tb, base, zp, zr1, zr2, rb, pp, pr1, pr2, ns, k32, k16, ks, qp, qr1, qr2, qf,
           kb, krow, qb, ss, rs, ls):
    dim = th.shape[1]
    nb = dim // BL
    me = lax.axis_index("feat")
    x, core = lax.div(me, 2), lax.rem(me, 2)
    ox, oc = 1 - x, 1 - core
    partner, cross = x * 2 + oc, ox * 2 + oc
    h = lax.rem(x + core, 2)
    oh = 1 - h

    def remote(src, dst, slot, dev):
        return pltpu.make_async_remote_copy(
            src_ref=src, dst_ref=dst, send_sem=ss.at[slot], recv_sem=rs.at[slot],
            device_id={"feat": dev}, device_id_type=MESH)

    def cols(b, size):
        return pl.ds(pl.multiple_of(b * size, size), size)

    def th_load(b):
        return pltpu.make_async_copy(th_hbm.at[:, cols(b, BL)], th.at[:, cols(b, BL)], ls.at[b])

    def a_load(c):
        return pltpu.make_async_copy(a_hbm.at[pl.ds(c * CH, CH)], a.at[pl.ds(c * CH, CH)], ls.at[nb + c])

    small = [pltpu.make_async_copy(src, dst, ls.at[nb + NC + i])
             for i, (src, dst) in enumerate([(lam_hbm, lam), (mu_hbm, mu), (u_hbm, u), (y_hbm, y)])]
    for b in range(nb):
        th_load(b).start()
    for c in range(NC):
        a_load(c).start()
    for cp in small:
        cp.start()

    barrier = pltpu.get_barrier_semaphore()
    for dev in (partner, cross):
        pl.semaphore_signal(barrier, inc=1, device_id={"feat": dev}, device_id_type=MESH)
    pl.semaphore_wait(barrier, 2)

    k32[...] = jnp.zeros_like(k32)

    def conv(b, carry):
        th_load(b).wait()
        tb[:, cols(b, BL)] = th[:, cols(b, BL)].astype(BF16)
        return carry

    lax.fori_loop(0, nb, conv, 0)
    for cp in small:
        cp.wait()

    ri = lax.broadcasted_iota(jnp.int32, (128, 128), 0)
    ci = lax.broadcasted_iota(jnp.int32, (128, 128), 1)
    eye, low = ri == ci, ri >= ci
    r64 = lax.broadcasted_iota(jnp.int32, (64, 128), 0)
    c64 = lax.broadcasted_iota(jnp.int32, (64, 128), 1)
    fold = (c64 < 64) & (r64 < c64)
    straight = ((ri < 64) & ((ci >= 64) | low)) | ((ri >= 64) & (ci > ri))
    r8 = lax.broadcasted_iota(jnp.int32, (8, 128), 0)

    def rows3(v):
        return jnp.where(r8 == 0, v[0], jnp.where(r8 == 1, v[1], jnp.where(r8 == 2, v[2], 0.0)))

    def to_col(row):
        return jnp.sum(jnp.where(eye, row, 0.0), axis=1, keepdims=True)

    def unpack(p, one):
        m10, m20, m21, mix, m2 = p[0:128], p[128:256], p[256:384], p[384:512], p[512:576]
        mix_t = mix.T
        d0 = jnp.where(low, mix, mix_t)
        d1 = jnp.where(ri < ci, mix, jnp.where(eye, one, mix_t))
        f = jnp.concatenate([m2, pltpu.roll(m2, 64, 1)], axis=0)
        d2 = jnp.where(straight, f, jnp.where(eye & (ri >= 64), one, f.T))
        return [[d0, m10.T, m20.T], [m10, d1, m21.T], [m20, m21, d2]]

    def step_body(step, carry):
        d2d_z = [remote(zp.at[c, oh], zr1.at[c], D2D_Z + c, partner) for c in range(NC)]
        ici_z = [remote(zp.at[c, h, ox], zr2.at[c], ICI_Z + c, cross) for c in range(NC)]
        ici_r = [remote(rb.at[c, h, x], rb.at[c, h, x], ICI_R + c, cross) for c in range(NC)]
        d2d_r = [remote(rb.at[c, h, x], rb.at[c, h, x], D2D_R + c, partner) for c in range(NC)]
        d2d_f = [remote(rb.at[c, h, ox], rb.at[c, h, ox], D2D_F + c, partner) for c in range(NC)]
        d2d_p = remote(pp.at[oh], pr1, D2D_P, partner)
        ici_p = remote(pp.at[h, ox], pr2, ICI_P, cross)
        ici_k = remote(k16.at[h, x], k16.at[h, x], ICI_K, cross)
        d2d_k = remote(k16.at[h, x], k16.at[h, x], D2D_K, partner)
        fwd_k = remote(k16.at[h, ox], k16.at[h, ox], FWD_K, partner)
        ici_s = remote(ks.at[h, x], ks.at[h, x], ICI_S, cross)
        d2d_s = remote(ks.at[h, x], ks.at[h, x], D2D_S, partner)
        fwd_s = remote(ks.at[h, ox], ks.at[h, ox], FWD_S, partner)
        d2d_q = remote(qp.at[oh], qr1, D2D_Q, partner)
        ici_q = remote(qp.at[h], qr2, ICI_Q, cross)
        d2d_qg = remote(qf.at[h], qf.at[h], D2D_QG, partner)

        def z_dot(c):
            @pl.when(step == 0)
            def _():
                a_load(c).wait()
                z = lax.dot_general(tb[...], a[pl.ds(c * CH, CH), :], DIMS_NT, preferred_element_type=F32)
                zp[c] = z.reshape(2, 2, OWN, CH)

            @pl.when(step > 0)
            def _():
                z = jnp.dot(tb[...], at[:, c * CH:(c + 1) * CH], preferred_element_type=F32)
                zp[c] = z.reshape(2, 2, OWN, CH)

            d2d_z[c].start()

        def a_transpose(c):
            @pl.when(step == 0)
            def _():
                def block(b, carry):
                    blk = cols(b, BL)
                    at[blk, c * CH:(c + 1) * CH] = a[c * CH:(c + 1) * CH, blk].T
                    return carry

                lax.fori_loop(0, dim // BL, block, 0)

        def z_chip(c):
            d2d_z[c].wait_recv()
            zp[c, h] = zp[c, h] + zr1[c]
            ici_z[c].start()

        def r_own(c):
            ici_z[c].wait_recv()
            z = zp[c, h, x] + zr2[c]
            n = CH // 128
            labels = jnp.concatenate([y[c * n + i:c * n + i + 1, :] for i in range(n)], axis=1)
            r = labels.astype(F32) - jax.nn.sigmoid(z)
            rb[c, h, x] = r.astype(BF16)
            ici_r[c].start()
            d2d_r[c].start()

        def r_forward(c):
            ici_r[c].wait_recv()
            d2d_f[c].start()

        def r_all(c):
            d2d_r[c].wait_recv()
            d2d_f[c].wait_recv()

        def gram():
            ga = lax.dot_general(tb[...], tb[0:256, :], DIMS_NT, preferred_element_type=F32)
            d2 = lax.dot_general(tb[256:384, :], tb[256:384, :], DIMS_NT, preferred_element_type=F32)
            d0, d1 = ga[0:128, 0:128], ga[128:256, 128:256]
            diag = rows3([jnp.sum(jnp.where(eye, d, 0.0), axis=0, keepdims=True) for d in (d0, d1, d2)])
            packed = jnp.concatenate(
                [ga[128:256, 0:128], ga[256:384, 0:128], ga[256:384, 128:256], jnp.where(low, d0, d1),
                 jnp.where(fold, pltpu.roll(d2[64:128], 64, 1), d2[0:64])], axis=0)
            for i in range(2):
                for j in range(2):
                    q = 2 * i + j
                    pp[i, j, 0:QR, :] = packed[QR * q:QR * (q + 1)]
                    pp[i, j, QR:QR + 8, :] = diag
            d2d_p.start()

        def gram_chip():
            d2d_p.wait_recv()
            pp[h] = pp[h] + pr1[...]
            ici_p.start()

        def kern_own():
            ici_p.wait_recv()
            pq = pp[h, x] + pr2[...]
            n_row = [pq[QR + i:QR + i + 1, :] for i in range(3)]
            n_col = [to_col(n) for n in n_row]
            pair = jnp.concatenate(
                [n_col[1] + n_row[0], n_col[2] + n_row[0], n_col[2] + n_row[1],
                 jnp.where(low, n_col[0] + n_row[0], n_col[1] + n_row[1]),
                 jnp.where(fold, n_col[2][64:128] + pltpu.roll(jnp.broadcast_to(n_row[2], (64, 128)), 64, 1),
                           n_col[2][0:64] + n_row[2])], axis=0)
            ns[...] = pair.reshape(2, 2, QR, 128)
            k = jnp.exp(-(jnp.maximum(ns[h, x] - 2.0 * pq[0:QR], 0.0) * inv_h))
            k16[h, x] = k.astype(BF16)
            ici_k.start()
            d2d_k.start()
            k32[h, x] = k
            part = unpack(k32[...].reshape(4 * QR, 128), 0.0)
            ks[h, x] = rows3([jnp.sum(part[0][j] + part[1][j] + part[2][j], axis=0, keepdims=True)
                              for j in range(3)])
            ici_s.start()
            d2d_s.start()

        def kern_forward():
            ici_k.wait_recv()
            fwd_k.start()
            ici_s.wait_recv()
            fwd_s.start()

        def kern_all():
            for cp in (d2d_k, fwd_k, d2d_s, fwd_s):
                cp.wait_recv()
            kmat = unpack(k16[...].reshape(4 * QR, 128).astype(F32), 1.0)
            total = (ks[0, 0] + ks[0, 1]) + (ks[1, 0] + ks[1, 1])
            lane = lax.broadcasted_iota(jnp.int32, (1, 128), 1)
            absent = [jnp.zeros((1, 128), F32), jnp.ones((1, 128), F32), jnp.where(lane >= 64, 1.0, 0.0)]
            for i in range(3):
                r = slice(128 * i, 128 * (i + 1))
                for j in range(3):
                    kb[r, 128 * j:128 * (j + 1)] = kmat[i][j].astype(BF16)
                kb[r, 384:512] = kmat[i][2].astype(BF16)
                krow[r, :] = jnp.broadcast_to(to_col(total[i:i + 1, :] + absent[i]), (128, 128))

        def proj():
            def block(b, acc):
                blk = cols(b, BQ)
                xb = (th[:, blk] - mu[:, blk]).astype(BF16)
                return acc + lax.dot_general(xb, u[:, blk], DIMS_NT, preferred_element_type=F32)

            q = lax.fori_loop(0, dim // BQ, block, jnp.zeros((NP, 16), F32))
            qp[...] = q.T.reshape(2, 8, NP)
            d2d_q.start()

        def proj_chip():
            d2d_q.wait_recv()
            qp[h] = qp[h] + qr1[...]
            ici_q.start()

        def proj_own():
            ici_q.wait_recv()
            qf[h] = qp[h] + qr2[...]
            d2d_qg.start()

        def prior():
            d2d_qg.wait_recv()
            qb[...] = qf[...].reshape(16, NP).T.astype(BF16)

            def block(b, carry):
                blk = cols(b, BB)
                low_rank = jnp.dot(qb[...], u[:, blk], preferred_element_type=F32)
                base[:, blk] = -((th[:, blk] - mu[:, blk]) * lam[:, blk]) - low_rank
                return carry

            lax.fori_loop(0, dim // BB, block, 0)

        def pull():
            def block(b, carry):
                blk = cols(b, BK)
                t = th[:, blk]
                pulled = jnp.dot(kb[:, 0:256], tb[0:256, blk], preferred_element_type=F32)
                th[:, blk] = t + c1 * (krow[:, 0:1] * t - pulled)
                return carry

            lax.fori_loop(0, dim // BK, block, 0)

        def likelihood(c):
            r_all(c)

            def block(b, carry):
                blk = cols(b, BR)
                ra = jnp.dot(rb[c].reshape(NP, CH), a[pl.ds(c * CH, CH), blk], preferred_element_type=F32)
                base[:, blk] = base[:, blk] + beta * ra
                return carry

            lax.fori_loop(0, dim // BR, block, 0)

        def update(c):
            r_all(c)

            def block(b, carry):
                blk = cols(b, BU)
                ra = jnp.dot(rb[c].reshape(NP, CH), a[pl.ds(c * CH, CH), blk], preferred_element_type=F32)
                s = (base[:, blk] + beta * ra).astype(BF16)
                rhs = jnp.concatenate([s, tb[256:384, blk] * (-two_h)], axis=0)
                t = th[:, blk] + c2 * jnp.dot(kb[...], rhs, preferred_element_type=F32)
                th[:, blk] = t
                tb[:, blk] = t.astype(BF16)
                return carry

            lax.fori_loop(0, dim // BU, block, 0)

        z_dot(0)
        gram()
        z_chip(0)
        z_dot(1)
        gram_chip()
        z_chip(1)
        proj()
        z_dot(2)
        proj_chip()
        a_transpose(0)
        kern_own()
        z_chip(2)
        a_transpose(1)
        proj_own()
        r_own(0)
        kern_forward()
        prior()
        r_own(1)
        a_transpose(2)
        kern_all()
        r_own(2)
        r_forward(0)
        pull()
        r_forward(1)
        likelihood(0)
        r_forward(2)
        likelihood(1)
        update(2)

        for cp in d2d_z + ici_z + ici_r + d2d_r + d2d_f + [
                d2d_p, ici_p, ici_k, d2d_k, fwd_k, ici_s, d2d_s, fwd_s, d2d_q, ici_q, d2d_qg]:
            cp.wait_send()
        return carry

    lax.fori_loop(0, NUM_STEPS, step_body, 0)


def solution(mesh):
    feat_size = mesh.shape["feat"]

    def local_run(particles, prec_diag, low_factor, prior_mean, data_mat, labels):
        n_part, dim_local = particles.shape
        dim_full = dim_local * feat_size
        m_rows = data_mat.shape[0]
        band_width = 2.0 * dim_full
        step_size = dim_full / 4.0
        beta = 2.0 / math.sqrt(m_rows * dim_full)
        c1 = step_size * (2.0 / band_width) / n_part
        c2 = step_size / n_part
        nb = dim_local // BL
        vm = pltpu.VMEM
        scratch = [
            vm((1, dim_local), F32),
            vm((1, dim_local), F32),
            vm((16, dim_local), BF16),
            vm((m_rows // 128, 128), jnp.int32),
            vm((MD, dim_local), BF16),
            vm((dim_local, MD), BF16),
            vm((NP, dim_local), BF16),
            vm((NP, dim_local), F32),
            vm((NC, 2, 2, OWN, CH), F32),
            vm((NC, 2, OWN, CH), F32),
            vm((NC, OWN, CH), F32),
            vm((NC, 2, 2, OWN, CH), BF16),
            vm((2, 2, QR + 8, 128), F32),
            vm((2, QR + 8, 128), F32),
            vm((QR + 8, 128), F32),
            vm((2, 2, QR, 128), F32),
            vm((2, 2, QR, 128), F32),
            vm((2, 2, QR, 128), BF16),
            vm((2, 2, 8, 128), F32),
            vm((2, 8, NP), F32),
            vm((8, NP), F32),
            vm((8, NP), F32),
            vm((2, 8, NP), F32),
            vm((NP, NP + 128), BF16),
            vm((NP, 128), F32),
            vm((NP, 16), BF16),
            pltpu.SemaphoreType.DMA((N_SEM,)),
            pltpu.SemaphoreType.DMA((N_SEM,)),
            pltpu.SemaphoreType.DMA((nb + NC + 4,)),
        ]
        hspec = pl.BlockSpec(memory_space=pltpu.HBM)
        vspec = pl.BlockSpec(memory_space=pltpu.VMEM)
        return pl.pallas_call(
            functools.partial(kernel, beta, c1, c2, 2.0 / band_width, 1.0 / band_width),
            out_shape=pltpu.VMEM((n_part, dim_local), F32),
            in_specs=[hspec] * 6,
            out_specs=vspec,
            scratch_shapes=scratch,
            compiler_params=pltpu.CompilerParams(
                collective_id=0, has_side_effects=True, vmem_limit_bytes=60_000_000),
            name="svgd",
        )(particles, prec_diag.reshape(1, dim_local), prior_mean.reshape(1, dim_local), low_factor.T,
          data_mat, labels.reshape(m_rows // 128, 128))

    return jax.shard_map(
        local_run,
        mesh=mesh,
        in_specs=(P("ens", "feat"), P(("ens", "feat")), P(("ens", "feat"), None),
                  P(("ens", "feat")), P("ens", "feat"), P("ens")),
        out_specs=P("ens", "feat"),
        check_vma=False,
    )
```

```python
import functools
import math

import jax
import jax.numpy as jnp
from jax import lax
from jax.experimental import pallas as pl
from jax.experimental.pallas import tpu as pltpu
from jax.sharding import PartitionSpec as P

NUM_STEPS = 3
DIMS_NT = (((1,), (1,)), ((), ()))
MESH = pl.DeviceIdType.MESH
F32 = jnp.float32
BF16 = jnp.bfloat16

NP = 384
MD = 768
CH = 256
NC = MD // CH
OWN = NP // 4
QR = 144
BL = 512
BQ = 4096
BB = 4096
BK = 4096
BR = 4096
BU = 4096
BO = 512

VMEM_STEPS = 43_000_000

D2D_Z, ICI_Z, ICI_R, D2D_R, D2D_F = 0, NC, 2 * NC, 3 * NC, 4 * NC
(D2D_P, ICI_P, ICI_K, D2D_K, FWD_K, ICI_S, D2D_S, FWD_S,
 D2D_Q, ICI_Q, D2D_QG) = range(5 * NC, 5 * NC + 11)
N_SEM = 5 * NC + 11


def chip_rows(chip):
    return pl.ds(pl.multiple_of(2 * OWN * chip, 2 * OWN), 2 * OWN)


def drive(beta, c2, two_h, th, base, a, tb, rb, c, chip, kx, j0, blk):
    ra = jnp.dot(rb[c, chip].reshape(2 * OWN, CH), a[pl.ds(c * CH, CH), blk], preferred_element_type=F32)
    s = (base[chip_rows(chip), blk] + beta * ra).astype(BF16)
    rhs = jnp.concatenate([s, tb[j0:j0 + 64, blk] * (-two_h)], axis=0)
    return th[:, blk] + c2 * jnp.dot(kx[...], rhs, preferred_element_type=F32)


def last_kernel(beta, c2, two_h, th, base, a, tb, rb, kb, out_hbm, out, sems):
    ox = 1 - lax.div(lax.axis_index("feat"), 2)
    copies = []
    for b in range(th.shape[1] // BO):
        blk = pl.ds(b * BO, BO)
        out[:, blk] = drive(beta, c2, two_h, th, base, a, tb, rb, NC - 1, ox, kb, 320, blk)
        copies.append(pltpu.make_async_copy(out.at[:, blk], out_hbm.at[:, blk], sems.at[b]))
        copies[-1].start()
    for cp in copies:
        cp.wait()


def kernel(beta, c1, c2, two_h, inv_h, th_hbm, lam_hbm, mu_hbm, u_hbm, a_hbm, y_hbm, th, base, a, tb, rb, kb,
           lam, mu, u, y, at, zp, zr1, zr2, pp, pr1, pr2, ns, k32, k16, ks, qp, qr1, qr2, qf,
           ka, kp, krow, qb, ss, rs, ls):
    dim = th.shape[1]
    nb = dim // BL
    me = lax.axis_index("feat")
    x, core = lax.div(me, 2), lax.rem(me, 2)
    ox, oc = 1 - x, 1 - core
    partner, cross = x * 2 + oc, ox * 2 + oc
    h = lax.rem(x + core, 2)
    oh = 1 - h

    def remote(src, dst, slot, dev):
        return pltpu.make_async_remote_copy(
            src_ref=src, dst_ref=dst, send_sem=ss.at[slot], recv_sem=rs.at[slot],
            device_id={"feat": dev}, device_id_type=MESH)

    def cols(b, size):
        return pl.ds(pl.multiple_of(b * size, size), size)

    def th_load(b):
        return pltpu.make_async_copy(th_hbm.at[:, cols(b, BL)], th.at[:, cols(b, BL)], ls.at[b])

    def a_load(c):
        return pltpu.make_async_copy(a_hbm.at[pl.ds(c * CH, CH)], a.at[pl.ds(c * CH, CH)], ls.at[nb + c])

    small = [pltpu.make_async_copy(src, dst, ls.at[nb + NC + i])
             for i, (src, dst) in enumerate([(lam_hbm, lam), (mu_hbm, mu), (u_hbm, u), (y_hbm, y)])]
    for b in range(nb):
        th_load(b).start()
    for c in range(NC):
        a_load(c).start()
    for cp in small:
        cp.start()

    barrier = pltpu.get_barrier_semaphore()
    for dev in (partner, cross):
        pl.semaphore_signal(barrier, inc=1, device_id={"feat": dev}, device_id_type=MESH)
    pl.semaphore_wait(barrier, 2)

    k32[...] = jnp.zeros_like(k32)

    def conv(b, carry):
        th_load(b).wait()
        tb[:, cols(b, BL)] = th[:, cols(b, BL)].astype(BF16)
        return carry

    lax.fori_loop(0, nb, conv, 0)
    for cp in small:
        cp.wait()

    ri = lax.broadcasted_iota(jnp.int32, (128, 128), 0)
    ci = lax.broadcasted_iota(jnp.int32, (128, 128), 1)
    eye, low, half = ri == ci, ri >= ci, ci < 64
    r64 = lax.broadcasted_iota(jnp.int32, (64, 128), 0)
    c64 = lax.broadcasted_iota(jnp.int32, (64, 128), 1)
    fold = (c64 < 64) & (r64 < c64)
    straight = ((ri < 64) & ((ci >= 64) | low)) | ((ri >= 64) & (ci > ri))
    r8 = lax.broadcasted_iota(jnp.int32, (8, 128), 0)

    def rows3(v):
        return jnp.where(r8 == 0, v[0], jnp.where(r8 == 1, v[1], jnp.where(r8 == 2, v[2], 0.0)))

    def to_col(row):
        return jnp.sum(jnp.where(eye, row, 0.0), axis=1, keepdims=True)

    def unpack(p, one):
        m10, m20, m21, mix, m2 = p[0:128], p[128:256], p[256:384], p[384:512], p[512:576]
        mix_t = mix.T
        d0 = jnp.where(low, mix, mix_t)
        d1 = jnp.where(ri < ci, mix, jnp.where(eye, one, mix_t))
        f = jnp.concatenate([m2, pltpu.roll(m2, 64, 1)], axis=0)
        d2 = jnp.where(straight, f, jnp.where(eye & (ri >= 64), one, f.T))
        return [[d0, m10.T, m20.T], [m10, d1, m21.T], [m20, m21, d2]]

    def step_body(step, carry):
        d2d_z = [remote(zp.at[c, :, oh], zr1.at[c], D2D_Z + c, partner) for c in range(NC)]
        ici_z = [remote(zp.at[c, ox, h], zr2.at[c], ICI_Z + c, cross) for c in range(NC)]
        ici_r = [remote(rb.at[c, x, h], rb.at[c, x, h], ICI_R + c, cross) for c in range(NC)]
        d2d_r = [remote(rb.at[c, x, h], rb.at[c, x, h], D2D_R + c, partner) for c in range(NC)]
        d2d_f = [remote(rb.at[c, ox, h], rb.at[c, ox, h], D2D_F + c, partner) for c in range(NC)]
        d2d_p = remote(pp.at[oh], pr1, D2D_P, partner)
        ici_p = remote(pp.at[h, ox], pr2, ICI_P, cross)
        ici_k = remote(k16.at[h, x], k16.at[h, x], ICI_K, cross)
        d2d_k = remote(k16.at[h, x], k16.at[h, x], D2D_K, partner)
        fwd_k = remote(k16.at[h, ox], k16.at[h, ox], FWD_K, partner)
        ici_s = remote(ks.at[h, x], ks.at[h, x], ICI_S, cross)
        d2d_s = remote(ks.at[h, x], ks.at[h, x], D2D_S, partner)
        fwd_s = remote(ks.at[h, ox], ks.at[h, ox], FWD_S, partner)
        d2d_q = remote(qp.at[oh], qr1, D2D_Q, partner)
        ici_q = remote(qp.at[h], qr2, ICI_Q, cross)
        d2d_qg = remote(qf.at[h], qf.at[h], D2D_QG, partner)

        def z_dot(c):
            @pl.when(step == 0)
            def _():
                a_load(c).wait()
                z = lax.dot_general(tb[...], a[pl.ds(c * CH, CH), :], DIMS_NT, preferred_element_type=F32)
                zp[c] = z.reshape(2, 2, OWN, CH)

            @pl.when(step > 0)
            def _():
                z = jnp.dot(tb[...], at[:, c * CH:(c + 1) * CH], preferred_element_type=F32)
                zp[c] = z.reshape(2, 2, OWN, CH)

            d2d_z[c].start()

        def z_dot_first(c):
            def rows(i):
                return jnp.concatenate([tb[pl.ds(pl.multiple_of((2 * j + i) * OWN, OWN), OWN), :] for j in range(2)], axis=0)

            @pl.when(step == 0)
            def _():
                a_load(c).wait()
                zp[c, :, oh] = lax.dot_general(rows(oh), a[pl.ds(c * CH, CH), :], DIMS_NT,
                                               preferred_element_type=F32).reshape(2, OWN, CH)
                d2d_z[c].start()
                zp[c, :, h] = lax.dot_general(rows(h), a[pl.ds(c * CH, CH), :], DIMS_NT,
                                              preferred_element_type=F32).reshape(2, OWN, CH)

            @pl.when(step > 0)
            def _():
                zp[c, :, oh] = jnp.dot(rows(oh), at[:, c * CH:(c + 1) * CH],
                                       preferred_element_type=F32).reshape(2, OWN, CH)
                d2d_z[c].start()
                zp[c, :, h] = jnp.dot(rows(h), at[:, c * CH:(c + 1) * CH],
                                      preferred_element_type=F32).reshape(2, OWN, CH)

        def a_transpose(c):
            @pl.when(step == 0)
            def _():
                def block(b, carry):
                    blk = cols(b, BL)
                    at[blk, c * CH:(c + 1) * CH] = a[c * CH:(c + 1) * CH, blk].T
                    return carry

                lax.fori_loop(0, dim // BL, block, 0)

        def z_chip(c):
            d2d_z[c].wait_recv()
            zp[c, :, h] = zp[c, :, h] + zr1[c]
            ici_z[c].start()

        def r_own(c):
            ici_z[c].wait_recv()
            z = zp[c, x, h] + zr2[c]
            n = CH // 128
            labels = jnp.concatenate([y[c * n + i:c * n + i + 1, :] for i in range(n)], axis=1)
            r = labels.astype(F32) - jax.nn.sigmoid(z)
            rb[c, x, h] = r.astype(BF16)
            ici_r[c].start()
            d2d_r[c].start()

        def r_forward(c):
            ici_r[c].wait_recv()
            d2d_f[c].start()

        def gram():
            ga = lax.dot_general(tb[...], tb[0:256, :], DIMS_NT, preferred_element_type=F32)
            d2 = lax.dot_general(tb[256:384, :], tb[256:384, :], DIMS_NT, preferred_element_type=F32)
            d0, d1 = ga[0:128, 0:128], ga[128:256, 128:256]
            diag = rows3([jnp.sum(jnp.where(eye, d, 0.0), axis=0, keepdims=True) for d in (d0, d1, d2)])
            packed = jnp.concatenate(
                [ga[128:256, 0:128], ga[256:384, 0:128], ga[256:384, 128:256], jnp.where(low, d0, d1),
                 jnp.where(fold, pltpu.roll(d2[64:128], 64, 1), d2[0:64])], axis=0)
            for i in range(2):
                for j in range(2):
                    q = 2 * i + j
                    pp[i, j, 0:QR, :] = packed[QR * q:QR * (q + 1)]
                    pp[i, j, QR:QR + 8, :] = diag
            d2d_p.start()

        def gram_chip():
            d2d_p.wait_recv()
            pp[h] = pp[h] + pr1[...]
            ici_p.start()

        def kern_own():
            ici_p.wait_recv()
            pq = pp[h, x] + pr2[...]
            n_row = [pq[QR + i:QR + i + 1, :] for i in range(3)]
            n_col = [to_col(n) for n in n_row]
            pair = jnp.concatenate(
                [n_col[1] + n_row[0], n_col[2] + n_row[0], n_col[2] + n_row[1],
                 jnp.where(low, n_col[0] + n_row[0], n_col[1] + n_row[1]),
                 jnp.where(fold, n_col[2][64:128] + pltpu.roll(jnp.broadcast_to(n_row[2], (64, 128)), 64, 1),
                           n_col[2][0:64] + n_row[2])], axis=0)
            ns[...] = pair.reshape(2, 2, QR, 128)
            k = jnp.exp(-(jnp.maximum(ns[h, x] - 2.0 * pq[0:QR], 0.0) * inv_h))
            k16[h, x] = k.astype(BF16)
            ici_k.start()
            d2d_k.start()
            k32[h, x] = k
            part = unpack(k32[...].reshape(4 * QR, 128), 0.0)
            ks[h, x] = rows3([jnp.sum(part[0][j] + part[1][j] + part[2][j], axis=0, keepdims=True)
                              for j in range(3)])
            ici_s.start()
            d2d_s.start()

        def kern_forward():
            ici_k.wait_recv()
            fwd_k.start()
            ici_s.wait_recv()
            fwd_s.start()

        def kern_all():
            for cp in (d2d_k, fwd_k, d2d_s, fwd_s):
                cp.wait_recv()
            kmat = unpack(k16[...].reshape(4 * QR, 128).astype(F32), 1.0)
            total = (ks[0, 0] + ks[0, 1]) + (ks[1, 0] + ks[1, 1])
            lane = lax.broadcasted_iota(jnp.int32, (1, 128), 1)
            absent = [jnp.zeros((1, 128), F32), jnp.ones((1, 128), F32), jnp.where(lane >= 64, 1.0, 0.0)]
            for i in range(3):
                r = slice(128 * i, 128 * (i + 1))
                k0, k1, k2 = kmat[i]
                s1, s2 = pltpu.roll(k1, 64, 1), pltpu.roll(k2, 64, 1)
                first = x == 0
                ka[r, :] = jnp.where(first, jnp.concatenate([k0, jnp.where(half, k1, s2)], axis=1),
                                     jnp.concatenate([jnp.where(half, s1, s2), s2], axis=1)).astype(BF16)
                kb[r, :] = jnp.where(first, jnp.concatenate([jnp.where(half, s1, s2), jnp.where(half, s2, k2)], axis=1),
                                     jnp.concatenate([k0, jnp.where(half, k1, k2)], axis=1)).astype(BF16)
                kp[r, :] = jnp.concatenate([k0, k1], axis=1).astype(BF16)
                krow[r, :] = jnp.broadcast_to(to_col(total[i:i + 1, :] + absent[i]), (128, 128))

        def proj():
            def block(b, acc):
                blk = cols(b, BQ)
                xb = (th[:, blk] - mu[:, blk]).astype(BF16)
                return acc + lax.dot_general(xb, u[:, blk], DIMS_NT, preferred_element_type=F32)

            q = lax.fori_loop(0, dim // BQ, block, jnp.zeros((NP, 16), F32))
            qp[...] = q.T.reshape(2, 8, NP)
            d2d_q.start()

        def proj_chip():
            d2d_q.wait_recv()
            qp[h] = qp[h] + qr1[...]
            ici_q.start()

        def proj_own():
            ici_q.wait_recv()
            qf[h] = qp[h] + qr2[...]
            d2d_qg.start()

        def prior():
            d2d_qg.wait_recv()
            qb[...] = qf[...].reshape(16, NP).T.astype(BF16)

            def block(b, carry):
                blk = cols(b, BB)
                low_rank = jnp.dot(qb[...], u[:, blk], preferred_element_type=F32)
                base[:, blk] = -((th[:, blk] - mu[:, blk]) * lam[:, blk]) - low_rank
                return carry

            lax.fori_loop(0, dim // BB, block, 0)

        def pull():
            def block(b, carry):
                blk = cols(b, BK)
                t = th[:, blk]
                pulled = jnp.dot(kp[...], tb[0:256, blk], preferred_element_type=F32)
                th[:, blk] = t + c1 * (krow[:, 0:1] * t - pulled)
                return carry

            lax.fori_loop(0, dim // BK, block, 0)

        def likelihood(c, chip):
            rows = chip_rows(chip)

            def block(b, carry):
                blk = cols(b, BR)
                ra = jnp.dot(rb[c, chip].reshape(2 * OWN, CH), a[pl.ds(c * CH, CH), blk], preferred_element_type=F32)
                base[rows, blk] = base[rows, blk] + beta * ra
                return carry

            lax.fori_loop(0, dim // BR, block, 0)

        def likelihood_near(c):
            d2d_r[c].wait_recv()
            likelihood(c, x)

        def likelihood_far(c):
            d2d_f[c].wait_recv()
            likelihood(c, ox)

        def update_near(c):
            d2d_r[c].wait_recv()

            def block(b, carry):
                blk = cols(b, BU)
                th[:, blk] = drive(beta, c2, two_h, th, base, a, tb, rb, c, x, ka, 256, blk)
                return carry

            lax.fori_loop(0, dim // BU, block, 0)

        def update_far(c):
            d2d_f[c].wait_recv()

            def block(b, carry):
                blk = cols(b, BU)
                t = drive(beta, c2, two_h, th, base, a, tb, rb, c, ox, kb, 320, blk)
                th[:, blk] = t
                tb[:, blk] = t.astype(BF16)
                return carry

            @pl.when(step < NUM_STEPS - 1)
            def _():
                lax.fori_loop(0, dim // BU, block, 0)

        z_dot(0)
        gram()
        z_chip(0)
        z_dot(1)
        proj()
        gram_chip()
        proj_chip()
        z_chip(1)
        z_dot(2)
        a_transpose(0)
        kern_own()
        proj_own()
        a_transpose(1)
        z_chip(2)
        r_own(0)
        prior()
        r_own(1)
        a_transpose(2)
        kern_forward()
        likelihood_near(0)
        likelihood_near(1)
        kern_all()
        r_own(2)
        pull()
        r_forward(0)
        update_near(2)
        r_forward(1)
        r_forward(2)
        likelihood_far(0)
        likelihood_far(1)
        update_far(2)

        for cp in d2d_z + ici_z + ici_r + d2d_r + d2d_f + [
                d2d_p, ici_p, ici_k, d2d_k, fwd_k, ici_s, d2d_s, fwd_s, d2d_q, ici_q, d2d_qg]:
            cp.wait_send()
        return carry

    lax.fori_loop(0, NUM_STEPS, step_body, 0)


def solution(mesh):
    feat_size = mesh.shape["feat"]

    def local_run(particles, prec_diag, low_factor, prior_mean, data_mat, labels):
        n_part, dim_local = particles.shape
        dim_full = dim_local * feat_size
        m_rows = data_mat.shape[0]
        band_width = 2.0 * dim_full
        step_size = dim_full / 4.0
        beta = 2.0 / math.sqrt(m_rows * dim_full)
        c1 = step_size * (2.0 / band_width) / n_part
        c2 = step_size / n_part
        nb = dim_local // BL
        vm = pltpu.VMEM
        scratch = [
            vm((1, dim_local), F32),
            vm((1, dim_local), F32),
            vm((16, dim_local), BF16),
            vm((m_rows // 128, 128), jnp.int32),
            vm((dim_local, MD), BF16),
            vm((NC, 2, 2, OWN, CH), F32),
            vm((NC, 2, OWN, CH), F32),
            vm((NC, OWN, CH), F32),
            vm((2, 2, QR + 8, 128), F32),
            vm((2, QR + 8, 128), F32),
            vm((QR + 8, 128), F32),
            vm((2, 2, QR, 128), F32),
            vm((2, 2, QR, 128), F32),
            vm((2, 2, QR, 128), BF16),
            vm((2, 2, 8, 128), F32),
            vm((2, 8, NP), F32),
            vm((8, NP), F32),
            vm((8, NP), F32),
            vm((2, 8, NP), F32),
            vm((NP, 256), BF16),
            vm((NP, 256), BF16),
            vm((NP, 128), F32),
            vm((NP, 16), BF16),
            pltpu.SemaphoreType.DMA((N_SEM,)),
            pltpu.SemaphoreType.DMA((N_SEM,)),
            pltpu.SemaphoreType.DMA((nb + NC + 4,)),
        ]
        hspec = pl.BlockSpec(memory_space=pltpu.HBM)
        vspec = pl.BlockSpec(memory_space=pltpu.VMEM)
        kept = pl.pallas_call(
            functools.partial(kernel, beta, c1, c2, 2.0 / band_width, 1.0 / band_width),
            out_shape=[
                vm((n_part, dim_local), F32),
                vm((n_part, dim_local), F32),
                vm((m_rows, dim_local), BF16),
                vm((n_part, dim_local), BF16),
                vm((NC, 2, 2, OWN, CH), BF16),
                vm((n_part, 256), BF16),
            ],
            in_specs=[hspec] * 6,
            out_specs=[vspec] * 6,
            scratch_shapes=scratch,
            compiler_params=pltpu.CompilerParams(
                collective_id=0, has_side_effects=True, vmem_limit_bytes=VMEM_STEPS),
            name="svgd",
        )(particles, prec_diag.reshape(1, dim_local), prior_mean.reshape(1, dim_local), low_factor.T,
          data_mat, labels.reshape(m_rows // 128, 128))
        return pl.pallas_call(
            functools.partial(last_kernel, beta, c2, 2.0 / band_width),
            out_shape=jax.ShapeDtypeStruct((n_part, dim_local), F32),
            in_specs=[vspec] * 6,
            out_specs=hspec,
            scratch_shapes=[vm((n_part, dim_local), F32), pltpu.SemaphoreType.DMA((dim_local // BO,))],
            compiler_params=pltpu.CompilerParams(vmem_limit_bytes=12 * 1024 * 1024),
            name="svgd_last",
        )(*kept)

    return jax.shard_map(
        local_run,
        mesh=mesh,
        in_specs=(P("ens", "feat"), P(("ens", "feat")), P(("ens", "feat"), None),
                  P(("ens", "feat")), P("ens", "feat"), P("ens")),
        out_specs=P("ens", "feat"),
        check_vma=False,
    )
```

```python
import functools
import math

import jax
import jax.numpy as jnp
from jax import lax
from jax.experimental import pallas as pl
from jax.experimental.pallas import tpu as pltpu
from jax.sharding import PartitionSpec as P

NUM_STEPS = 3
DIMS_NT = (((1,), (1,)), ((), ()))
MESH = pl.DeviceIdType.MESH
F32 = jnp.float32
BF16 = jnp.bfloat16

NP = 384
MD = 768
CH = 256
NC = MD // CH
OWN = NP // 4
QR = 144
BL = 512
BQ = 4096
BB = 4096
BK = 4096
BR = 4096
BU = 4096
NF = 4
BO = 1024

VMEM_STEPS = 43_000_000

D2D_Z, ICI_Z, ICI_R, D2D_R, D2D_F = 0, NC, 2 * NC, 3 * NC, 4 * NC
(D2D_P, ICI_P, ICI_K, D2D_K, FWD_K, ICI_S, D2D_S, FWD_S,
 D2D_Q, ICI_Q, D2D_QG) = range(5 * NC, 5 * NC + 11)
N_SEM = 5 * NC + 11


def chip_rows(chip):
    return pl.ds(pl.multiple_of(2 * OWN * chip, 2 * OWN), 2 * OWN)


def drive(beta, c2, two_h, th, base, a, tb, rb, c, chip, kx, j0, blk):
    ra = jnp.dot(rb[c, chip].reshape(2 * OWN, CH), a[pl.ds(c * CH, CH), blk], preferred_element_type=F32)
    s = (base[chip_rows(chip), blk] + beta * ra).astype(BF16)
    rhs = jnp.concatenate([s, tb[j0:j0 + 64, blk] * (-two_h)], axis=0)
    return th[:, blk] + c2 * jnp.dot(kx[...], rhs, preferred_element_type=F32)


def last_kernel(beta, c2, two_h, th, base, a, tb, rb, kb, out_hbm, out, sems):
    ox = 1 - lax.div(lax.axis_index("feat"), 2)
    copies = []
    for b in range(th.shape[1] // BO):
        blk = pl.ds(b * BO, BO)
        out[:, blk] = drive(beta, c2, two_h, th, base, a, tb, rb, NC - 1, ox, kb, 320, blk)
        copies.append(pltpu.make_async_copy(out.at[:, blk], out_hbm.at[:, blk], sems.at[b]))
        copies[-1].start()
    for cp in copies:
        cp.wait()


def kernel(beta, c1, c2, two_h, inv_h, th_hbm, lam_hbm, mu_hbm, u_hbm, a_hbm, y_hbm, th, base, a, tb, rb, kb,
           lam, mu, u, y, at, zp, zr1, zr2, pp, pr1, pr2, ns, k32, k16, ks, qp, qr1, qr2, qf,
           ka, kp, krow, qb, ss, rs, ls):
    dim = th.shape[1]
    nb = dim // BL
    me = lax.axis_index("feat")
    x, core = lax.div(me, 2), lax.rem(me, 2)
    ox, oc = 1 - x, 1 - core
    partner, cross = x * 2 + oc, ox * 2 + oc
    h = lax.rem(x + core, 2)
    oh = 1 - h

    def remote(src, dst, slot, dev):
        return pltpu.make_async_remote_copy(
            src_ref=src, dst_ref=dst, send_sem=ss.at[slot], recv_sem=rs.at[slot],
            device_id={"feat": dev}, device_id_type=MESH)

    def cols(b, size):
        return pl.ds(pl.multiple_of(b * size, size), size)

    def th_load(b):
        return pltpu.make_async_copy(th_hbm.at[:, cols(b, BL)], th.at[:, cols(b, BL)], ls.at[b])

    def a_load(c):
        return pltpu.make_async_copy(a_hbm.at[pl.ds(c * CH, CH)], a.at[pl.ds(c * CH, CH)], ls.at[nb + c])

    small = [pltpu.make_async_copy(src, dst, ls.at[nb + NC + i])
             for i, (src, dst) in enumerate([(lam_hbm, lam), (mu_hbm, mu), (u_hbm, u), (y_hbm, y)])]
    def a_first(i):
        part = pl.ds(i * (dim // NF), dim // NF)
        return pltpu.make_async_copy(a_hbm.at[pl.ds(0, CH), part], a.at[pl.ds(0, CH), part], ls.at[nb + NC + 4 + i])

    for i in range(NF):
        for b in range(i * nb // NF, (i + 1) * nb // NF):
            th_load(b).start()
        a_first(i).start()
    for cp in small:
        cp.start()

    barrier = pltpu.get_barrier_semaphore()
    for dev in (partner, cross):
        pl.semaphore_signal(barrier, inc=1, device_id={"feat": dev}, device_id_type=MESH)
    pl.semaphore_wait(barrier, 2)

    k32[...] = jnp.zeros_like(k32)

    def conv(b, carry):
        th_load(b).wait()
        tb[:, cols(b, BL)] = th[:, cols(b, BL)].astype(BF16)
        return carry

    for i in range(NF):
        part = slice(i * (dim // NF), (i + 1) * (dim // NF))
        lax.fori_loop(i * nb // NF, (i + 1) * nb // NF, conv, 0)
        a_first(i).wait()
        if i == NF - 1:
            for c in range(1, NC):
                a_load(c).start()
        z = lax.dot_general(tb[:, part], a[0:CH, part], DIMS_NT, preferred_element_type=F32).reshape(2, 2, OWN, CH)
        zp[0] = z if i == 0 else zp[0] + z
    for cp in small:
        cp.wait()

    ri = lax.broadcasted_iota(jnp.int32, (128, 128), 0)
    ci = lax.broadcasted_iota(jnp.int32, (128, 128), 1)
    eye, low, half = ri == ci, ri >= ci, ci < 64
    r64 = lax.broadcasted_iota(jnp.int32, (64, 128), 0)
    c64 = lax.broadcasted_iota(jnp.int32, (64, 128), 1)
    fold = (c64 < 64) & (r64 < c64)
    straight = ((ri < 64) & ((ci >= 64) | low)) | ((ri >= 64) & (ci > ri))
    r8 = lax.broadcasted_iota(jnp.int32, (8, 128), 0)

    def rows3(v):
        return jnp.where(r8 == 0, v[0], jnp.where(r8 == 1, v[1], jnp.where(r8 == 2, v[2], 0.0)))

    def to_col(row):
        return jnp.sum(jnp.where(eye, row, 0.0), axis=1, keepdims=True)

    def unpack(p, one):
        m10, m20, m21, mix, m2 = p[0:128], p[128:256], p[256:384], p[384:512], p[512:576]
        mix_t = mix.T
        d0 = jnp.where(low, mix, mix_t)
        d1 = jnp.where(ri < ci, mix, jnp.where(eye, one, mix_t))
        f = jnp.concatenate([m2, pltpu.roll(m2, 64, 1)], axis=0)
        d2 = jnp.where(straight, f, jnp.where(eye & (ri >= 64), one, f.T))
        return [[d0, m10.T, m20.T], [m10, d1, m21.T], [m20, m21, d2]]

    def step_body(step, carry):
        d2d_z = [remote(zp.at[c, :, oh], zr1.at[c], D2D_Z + c, partner) for c in range(NC)]
        ici_z = [remote(zp.at[c, ox, h], zr2.at[c], ICI_Z + c, cross) for c in range(NC)]
        ici_r = [remote(rb.at[c, x, h], rb.at[c, x, h], ICI_R + c, cross) for c in range(NC)]
        d2d_r = [remote(rb.at[c, x, h], rb.at[c, x, h], D2D_R + c, partner) for c in range(NC)]
        d2d_f = [remote(rb.at[c, ox, h], rb.at[c, ox, h], D2D_F + c, partner) for c in range(NC)]
        d2d_p = remote(pp.at[oh], pr1, D2D_P, partner)
        ici_p = remote(pp.at[h, ox], pr2, ICI_P, cross)
        ici_k = remote(k16.at[h, x], k16.at[h, x], ICI_K, cross)
        d2d_k = remote(k16.at[h, x], k16.at[h, x], D2D_K, partner)
        fwd_k = remote(k16.at[h, ox], k16.at[h, ox], FWD_K, partner)
        ici_s = remote(ks.at[h, x], ks.at[h, x], ICI_S, cross)
        d2d_s = remote(ks.at[h, x], ks.at[h, x], D2D_S, partner)
        fwd_s = remote(ks.at[h, ox], ks.at[h, ox], FWD_S, partner)
        d2d_q = remote(qp.at[oh], qr1, D2D_Q, partner)
        ici_q = remote(qp.at[h], qr2, ICI_Q, cross)
        d2d_qg = remote(qf.at[h], qf.at[h], D2D_QG, partner)

        def z_dot(c):
            if c > 0:
                @pl.when(step == 0)
                def _():
                    a_load(c).wait()
                    z = lax.dot_general(tb[...], a[pl.ds(c * CH, CH), :], DIMS_NT, preferred_element_type=F32)
                    zp[c] = z.reshape(2, 2, OWN, CH)

            @pl.when(step > 0)
            def _():
                z = jnp.dot(tb[...], at[:, c * CH:(c + 1) * CH], preferred_element_type=F32)
                zp[c] = z.reshape(2, 2, OWN, CH)

            d2d_z[c].start()

        def a_transpose(c):
            @pl.when(step == 0)
            def _():
                def block(b, carry):
                    blk = cols(b, BL)
                    at[blk, c * CH:(c + 1) * CH] = a[c * CH:(c + 1) * CH, blk].T
                    return carry

                lax.fori_loop(0, dim // BL, block, 0)

        def z_chip(c):
            d2d_z[c].wait_recv()
            zp[c, :, h] = zp[c, :, h] + zr1[c]
            ici_z[c].start()

        def r_own(c):
            ici_z[c].wait_recv()
            z = zp[c, x, h] + zr2[c]
            n = CH // 128
            labels = jnp.concatenate([y[c * n + i:c * n + i + 1, :] for i in range(n)], axis=1)
            r = labels.astype(F32) - jax.nn.sigmoid(z)
            rb[c, x, h] = r.astype(BF16)
            ici_r[c].start()
            d2d_r[c].start()

        def r_forward(c):
            ici_r[c].wait_recv()
            d2d_f[c].start()

        def gram():
            ga = lax.dot_general(tb[...], tb[0:256, :], DIMS_NT, preferred_element_type=F32)
            d2 = lax.dot_general(tb[256:384, :], tb[256:384, :], DIMS_NT, preferred_element_type=F32)
            d0, d1 = ga[0:128, 0:128], ga[128:256, 128:256]
            diag = rows3([jnp.sum(jnp.where(eye, d, 0.0), axis=0, keepdims=True) for d in (d0, d1, d2)])
            packed = jnp.concatenate(
                [ga[128:256, 0:128], ga[256:384, 0:128], ga[256:384, 128:256], jnp.where(low, d0, d1),
                 jnp.where(fold, pltpu.roll(d2[64:128], 64, 1), d2[0:64])], axis=0)
            for i in range(2):
                for j in range(2):
                    q = 2 * i + j
                    pp[i, j, 0:QR, :] = packed[QR * q:QR * (q + 1)]
                    pp[i, j, QR:QR + 8, :] = diag
            d2d_p.start()

        def gram_chip():
            d2d_p.wait_recv()
            pp[h] = pp[h] + pr1[...]
            ici_p.start()

        def kern_own():
            ici_p.wait_recv()
            pq = pp[h, x] + pr2[...]
            n_row = [pq[QR + i:QR + i + 1, :] for i in range(3)]
            n_col = [to_col(n) for n in n_row]
            pair = jnp.concatenate(
                [n_col[1] + n_row[0], n_col[2] + n_row[0], n_col[2] + n_row[1],
                 jnp.where(low, n_col[0] + n_row[0], n_col[1] + n_row[1]),
                 jnp.where(fold, n_col[2][64:128] + pltpu.roll(jnp.broadcast_to(n_row[2], (64, 128)), 64, 1),
                           n_col[2][0:64] + n_row[2])], axis=0)
            ns[...] = pair.reshape(2, 2, QR, 128)
            k = jnp.exp(-(jnp.maximum(ns[h, x] - 2.0 * pq[0:QR], 0.0) * inv_h))
            k16[h, x] = k.astype(BF16)
            ici_k.start()
            d2d_k.start()
            k32[h, x] = k
            part = unpack(k32[...].reshape(4 * QR, 128), 0.0)
            ks[h, x] = rows3([jnp.sum(part[0][j] + part[1][j] + part[2][j], axis=0, keepdims=True)
                              for j in range(3)])
            ici_s.start()
            d2d_s.start()

        def kern_forward():
            ici_k.wait_recv()
            fwd_k.start()
            ici_s.wait_recv()
            fwd_s.start()

        def kern_all():
            for cp in (d2d_k, fwd_k, d2d_s, fwd_s):
                cp.wait_recv()
            kmat = unpack(k16[...].reshape(4 * QR, 128).astype(F32), 1.0)
            total = (ks[0, 0] + ks[0, 1]) + (ks[1, 0] + ks[1, 1])
            lane = lax.broadcasted_iota(jnp.int32, (1, 128), 1)
            absent = [jnp.zeros((1, 128), F32), jnp.ones((1, 128), F32), jnp.where(lane >= 64, 1.0, 0.0)]
            for i in range(3):
                r = slice(128 * i, 128 * (i + 1))
                k0, k1, k2 = kmat[i]
                s1, s2 = pltpu.roll(k1, 64, 1), pltpu.roll(k2, 64, 1)
                first = x == 0
                ka[r, :] = jnp.where(first, jnp.concatenate([k0, jnp.where(half, k1, s2)], axis=1),
                                     jnp.concatenate([jnp.where(half, s1, s2), s2], axis=1)).astype(BF16)
                kb[r, :] = jnp.where(first, jnp.concatenate([jnp.where(half, s1, s2), jnp.where(half, s2, k2)], axis=1),
                                     jnp.concatenate([k0, jnp.where(half, k1, k2)], axis=1)).astype(BF16)
                kp[r, :] = jnp.concatenate([k0, k1], axis=1).astype(BF16)
                krow[r, :] = jnp.broadcast_to(to_col(total[i:i + 1, :] + absent[i]), (128, 128))

        def proj():
            def block(b, acc):
                blk = cols(b, BQ)
                xb = (th[:, blk] - mu[:, blk]).astype(BF16)
                return acc + lax.dot_general(xb, u[:, blk], DIMS_NT, preferred_element_type=F32)

            q = lax.fori_loop(0, dim // BQ, block, jnp.zeros((NP, 16), F32))
            qp[...] = q.T.reshape(2, 8, NP)
            d2d_q.start()

        def proj_chip():
            d2d_q.wait_recv()
            qp[h] = qp[h] + qr1[...]
            ici_q.start()

        def proj_own():
            ici_q.wait_recv()
            qf[h] = qp[h] + qr2[...]
            d2d_qg.start()

        def prior():
            d2d_qg.wait_recv()
            qb[...] = qf[...].reshape(16, NP).T.astype(BF16)

            def block(b, carry):
                blk = cols(b, BB)
                low_rank = jnp.dot(qb[...], u[:, blk], preferred_element_type=F32)
                base[:, blk] = -((th[:, blk] - mu[:, blk]) * lam[:, blk]) - low_rank
                return carry

            lax.fori_loop(0, dim // BB, block, 0)

        def pull():
            def block(b, carry):
                blk = cols(b, BK)
                t = th[:, blk]
                pulled = jnp.dot(kp[...], tb[0:256, blk], preferred_element_type=F32)
                th[:, blk] = t + c1 * (krow[:, 0:1] * t - pulled)
                return carry

            lax.fori_loop(0, dim // BK, block, 0)

        def likelihood(c, chip):
            rows = chip_rows(chip)

            def block(b, carry):
                blk = cols(b, BR)
                ra = jnp.dot(rb[c, chip].reshape(2 * OWN, CH), a[pl.ds(c * CH, CH), blk], preferred_element_type=F32)
                base[rows, blk] = base[rows, blk] + beta * ra
                return carry

            lax.fori_loop(0, dim // BR, block, 0)

        def likelihood_near(c):
            d2d_r[c].wait_recv()
            likelihood(c, x)

        def likelihood_far(c):
            d2d_f[c].wait_recv()
            likelihood(c, ox)

        def update_near(c):
            d2d_r[c].wait_recv()

            def block(b, carry):
                blk = cols(b, BU)
                th[:, blk] = drive(beta, c2, two_h, th, base, a, tb, rb, c, x, ka, 256, blk)
                return carry

            lax.fori_loop(0, dim // BU, block, 0)

        def update_far(c):
            d2d_f[c].wait_recv()

            def block(b, carry):
                blk = cols(b, BU)
                t = drive(beta, c2, two_h, th, base, a, tb, rb, c, ox, kb, 320, blk)
                th[:, blk] = t
                tb[:, blk] = t.astype(BF16)
                return carry

            @pl.when(step < NUM_STEPS - 1)
            def _():
                lax.fori_loop(0, dim // BU, block, 0)

        z_dot(0)
        gram()
        z_chip(0)
        z_dot(1)
        proj()
        gram_chip()
        proj_chip()
        z_chip(1)
        z_dot(2)
        a_transpose(0)
        kern_own()
        proj_own()
        a_transpose(1)
        z_chip(2)
        r_own(0)
        prior()
        r_own(1)
        a_transpose(2)
        kern_forward()
        likelihood_near(0)
        likelihood_near(1)
        kern_all()
        r_own(2)
        pull()
        r_forward(0)
        update_near(2)
        r_forward(1)
        r_forward(2)
        likelihood_far(0)
        likelihood_far(1)
        update_far(2)

        for cp in d2d_z + ici_z + ici_r + d2d_r + d2d_f + [
                d2d_p, ici_p, ici_k, d2d_k, fwd_k, ici_s, d2d_s, fwd_s, d2d_q, ici_q, d2d_qg]:
            cp.wait_send()
        return carry

    lax.fori_loop(0, NUM_STEPS, step_body, 0)


def solution(mesh):
    feat_size = mesh.shape["feat"]

    def local_run(particles, prec_diag, low_factor, prior_mean, data_mat, labels):
        n_part, dim_local = particles.shape
        dim_full = dim_local * feat_size
        m_rows = data_mat.shape[0]
        band_width = 2.0 * dim_full
        step_size = dim_full / 4.0
        beta = 2.0 / math.sqrt(m_rows * dim_full)
        c1 = step_size * (2.0 / band_width) / n_part
        c2 = step_size / n_part
        nb = dim_local // BL
        vm = pltpu.VMEM
        scratch = [
            vm((1, dim_local), F32),
            vm((1, dim_local), F32),
            vm((16, dim_local), BF16),
            vm((m_rows // 128, 128), jnp.int32),
            vm((dim_local, MD), BF16),
            vm((NC, 2, 2, OWN, CH), F32),
            vm((NC, 2, OWN, CH), F32),
            vm((NC, OWN, CH), F32),
            vm((2, 2, QR + 8, 128), F32),
            vm((2, QR + 8, 128), F32),
            vm((QR + 8, 128), F32),
            vm((2, 2, QR, 128), F32),
            vm((2, 2, QR, 128), F32),
            vm((2, 2, QR, 128), BF16),
            vm((2, 2, 8, 128), F32),
            vm((2, 8, NP), F32),
            vm((8, NP), F32),
            vm((8, NP), F32),
            vm((2, 8, NP), F32),
            vm((NP, 256), BF16),
            vm((NP, 256), BF16),
            vm((NP, 128), F32),
            vm((NP, 16), BF16),
            pltpu.SemaphoreType.DMA((N_SEM,)),
            pltpu.SemaphoreType.DMA((N_SEM,)),
            pltpu.SemaphoreType.DMA((nb + NC + 4 + NF,)),
        ]
        hspec = pl.BlockSpec(memory_space=pltpu.HBM)
        vspec = pl.BlockSpec(memory_space=pltpu.VMEM)
        kept = pl.pallas_call(
            functools.partial(kernel, beta, c1, c2, 2.0 / band_width, 1.0 / band_width),
            out_shape=[
                vm((n_part, dim_local), F32),
                vm((n_part, dim_local), F32),
                vm((m_rows, dim_local), BF16),
                vm((n_part, dim_local), BF16),
                vm((NC, 2, 2, OWN, CH), BF16),
                vm((n_part, 256), BF16),
            ],
            in_specs=[hspec] * 6,
            out_specs=[vspec] * 6,
            scratch_shapes=scratch,
            compiler_params=pltpu.CompilerParams(
                collective_id=0, has_side_effects=True, vmem_limit_bytes=VMEM_STEPS),
            name="svgd",
        )(particles, prec_diag.reshape(1, dim_local), prior_mean.reshape(1, dim_local), low_factor.T,
          data_mat, labels.reshape(m_rows // 128, 128))
        return pl.pallas_call(
            functools.partial(last_kernel, beta, c2, 2.0 / band_width),
            out_shape=jax.ShapeDtypeStruct((n_part, dim_local), F32),
            in_specs=[vspec] * 6,
            out_specs=hspec,
            scratch_shapes=[vm((n_part, dim_local), F32), pltpu.SemaphoreType.DMA((dim_local // BO,))],
            compiler_params=pltpu.CompilerParams(vmem_limit_bytes=12 * 1024 * 1024),
            name="svgd_last",
        )(*kept)

    return jax.shard_map(
        local_run,
        mesh=mesh,
        in_specs=(P("ens", "feat"), P(("ens", "feat")), P(("ens", "feat"), None),
                  P(("ens", "feat")), P("ens", "feat"), P("ens")),
        out_specs=P("ens", "feat"),
        check_vma=False,
    )
```

```python
import functools
import math

import jax
import jax.numpy as jnp
from jax import lax
from jax.experimental import pallas as pl
from jax.experimental.pallas import tpu as pltpu
from jax.sharding import PartitionSpec as P

NUM_STEPS = 3
DIMS_NT = (((1,), (1,)), ((), ()))
MESH = pl.DeviceIdType.MESH
F32 = jnp.float32
BF16 = jnp.bfloat16

NP = 384
MD = 768
CH = 256
NC = MD // CH
OWN = NP // 4
QR = 144
BL = 512
BQ = 4096
BB = 2048
BK = 4096
BR = 4096
BU = 4096
NF = 4
BO = 1024

VMEM_STEPS = 43_000_000

D2D_Z, ICI_Z, ICI_R, D2D_R, D2D_F = 0, NC, 2 * NC, 3 * NC, 4 * NC
(D2D_P, ICI_P, ICI_K, D2D_K, FWD_K, ICI_S, D2D_S, FWD_S,
 D2D_Q, ICI_Q, D2D_QG) = range(5 * NC, 5 * NC + 11)
N_SEM = 5 * NC + 11


def chip_rows(chip):
    return pl.ds(pl.multiple_of(2 * OWN * chip, 2 * OWN), 2 * OWN)


def drive(beta, c2, two_h, th, base, a, tb, rb, c, chip, kx, j0, blk):
    ra = jnp.dot(rb[c, chip].reshape(2 * OWN, CH), a[pl.ds(c * CH, CH), blk], preferred_element_type=F32)
    s = (base[chip_rows(chip), blk] + beta * ra).astype(BF16)
    rhs = jnp.concatenate([s, tb[j0:j0 + 64, blk] * (-two_h)], axis=0)
    return th[:, blk] + c2 * jnp.dot(kx[...], rhs, preferred_element_type=F32)


def last_kernel(beta, c2, two_h, th, base, a, tb, rb, kb, out_hbm, out, sems):
    ox = 1 - lax.div(lax.axis_index("feat"), 2)
    copies = []
    for b in range(th.shape[1] // BO):
        blk = pl.ds(b * BO, BO)
        out[:, blk] = drive(beta, c2, two_h, th, base, a, tb, rb, NC - 1, ox, kb, 320, blk)
        copies.append(pltpu.make_async_copy(out.at[:, blk], out_hbm.at[:, blk], sems.at[b]))
        copies[-1].start()
    for cp in copies:
        cp.wait()


def kernel(beta, c1, c2, two_h, inv_h, th_hbm, lam_hbm, mu_hbm, u_hbm, a_hbm, y_hbm, th, base, a, tb, rb, kb,
           lam, mu, u, y, at, zp, zr1, zr2, pp, pr1, pr2, ns, k32, k16, ks, qp, qr1, qr2, qf,
           ka, kp, krow, qb, ss, rs, ls):
    dim = th.shape[1]
    nb = dim // BL
    me = lax.axis_index("feat")
    x, core = lax.div(me, 2), lax.rem(me, 2)
    ox, oc = 1 - x, 1 - core
    partner, cross, peer = x * 2 + oc, ox * 2 + oc, ox * 2 + core
    h = lax.rem(x + core, 2)
    oh = 1 - h

    def remote(src, dst, slot, dev):
        return pltpu.make_async_remote_copy(
            src_ref=src, dst_ref=dst, send_sem=ss.at[slot], recv_sem=rs.at[slot],
            device_id={"feat": dev}, device_id_type=MESH)

    def cols(b, size):
        return pl.ds(pl.multiple_of(b * size, size), size)

    def th_load(b):
        return pltpu.make_async_copy(th_hbm.at[:, cols(b, BL)], th.at[:, cols(b, BL)], ls.at[b])

    def a_load(c):
        return pltpu.make_async_copy(a_hbm.at[pl.ds(c * CH, CH)], a.at[pl.ds(c * CH, CH)], ls.at[nb + c])

    small = [pltpu.make_async_copy(src, dst, ls.at[nb + NC + i])
             for i, (src, dst) in enumerate([(lam_hbm, lam), (mu_hbm, mu), (u_hbm, u), (y_hbm, y)])]
    def a_first(i):
        part = pl.ds(i * (dim // NF), dim // NF)
        return pltpu.make_async_copy(a_hbm.at[pl.ds(0, CH), part], a.at[pl.ds(0, CH), part], ls.at[nb + NC + 4 + i])

    for i in range(NF):
        for b in range(i * nb // NF, (i + 1) * nb // NF):
            th_load(b).start()
        a_first(i).start()
    for cp in small:
        cp.start()

    barrier = pltpu.get_barrier_semaphore()
    for dev in (partner, cross, peer):
        pl.semaphore_signal(barrier, inc=1, device_id={"feat": dev}, device_id_type=MESH)
    pl.semaphore_wait(barrier, 3)

    k32[...] = jnp.zeros_like(k32)

    def conv(b, carry):
        th_load(b).wait()
        tb[:, cols(b, BL)] = th[:, cols(b, BL)].astype(BF16)
        return carry

    for i in range(NF):
        part = slice(i * (dim // NF), (i + 1) * (dim // NF))
        lax.fori_loop(i * nb // NF, (i + 1) * nb // NF, conv, 0)
        a_first(i).wait()
        if i == NF - 1:
            for c in range(1, NC):
                a_load(c).start()
        z = lax.dot_general(tb[:, part], a[0:CH, part], DIMS_NT, preferred_element_type=F32).reshape(2, 2, OWN, CH)
        zp[0] = z if i == 0 else zp[0] + z
    for cp in small:
        cp.wait()

    ri = lax.broadcasted_iota(jnp.int32, (128, 128), 0)
    ci = lax.broadcasted_iota(jnp.int32, (128, 128), 1)
    eye, low, half = ri == ci, ri >= ci, ci < 64
    r64 = lax.broadcasted_iota(jnp.int32, (64, 128), 0)
    c64 = lax.broadcasted_iota(jnp.int32, (64, 128), 1)
    fold = (c64 < 64) & (r64 < c64)
    straight = ((ri < 64) & ((ci >= 64) | low)) | ((ri >= 64) & (ci > ri))
    r8 = lax.broadcasted_iota(jnp.int32, (8, 128), 0)

    def rows3(v):
        return jnp.where(r8 == 0, v[0], jnp.where(r8 == 1, v[1], jnp.where(r8 == 2, v[2], 0.0)))

    def to_col(row):
        return jnp.sum(jnp.where(eye, row, 0.0), axis=1, keepdims=True)

    def unpack(p, one):
        m10, m20, m21, mix, m2 = p[0:128], p[128:256], p[256:384], p[384:512], p[512:576]
        mix_t = mix.T
        d0 = jnp.where(low, mix, mix_t)
        d1 = jnp.where(ri < ci, mix, jnp.where(eye, one, mix_t))
        f = jnp.concatenate([m2, pltpu.roll(m2, 64, 1)], axis=0)
        d2 = jnp.where(straight, f, jnp.where(eye & (ri >= 64), one, f.T))
        return [[d0, m10.T, m20.T], [m10, d1, m21.T], [m20, m21, d2]]

    def step_body(step, carry):
        d2d_z = [remote(zp.at[c, :, oh], zr1.at[c], D2D_Z + c, partner) for c in range(NC)]
        ici_z = [remote(zp.at[c, ox, h], zr2.at[c], ICI_Z + c, cross) for c in range(NC)]
        ici_r = [remote(rb.at[c, x, h], rb.at[c, x, h], ICI_R + c, cross) for c in range(NC)]
        d2d_r = [remote(rb.at[c, x, h], rb.at[c, x, h], D2D_R + c, partner) for c in range(NC)]
        d2d_f = [remote(rb.at[c, ox, h], rb.at[c, ox, h], D2D_F + c, partner) for c in range(NC - 1)]
        ici_b = remote(rb.at[NC - 1, x, h], rb.at[NC - 1, x, h], D2D_F + NC - 1, peer)
        d2d_p = remote(pp.at[oh], pr1, D2D_P, partner)
        ici_p = remote(pp.at[h, ox], pr2, ICI_P, cross)
        ici_k = remote(k16.at[h, x], k16.at[h, x], ICI_K, cross)
        d2d_k = remote(k16.at[h, x], k16.at[h, x], D2D_K, partner)
        fwd_k = remote(k16.at[h, ox], k16.at[h, ox], FWD_K, partner)
        ici_s = remote(ks.at[h, x], ks.at[h, x], ICI_S, cross)
        d2d_s = remote(ks.at[h, x], ks.at[h, x], D2D_S, partner)
        fwd_s = remote(ks.at[h, ox], ks.at[h, ox], FWD_S, partner)
        d2d_q = remote(qp.at[oh], qr1, D2D_Q, partner)
        ici_q = remote(qp.at[h], qr2, ICI_Q, cross)
        d2d_qg = remote(qf.at[h], qf.at[h], D2D_QG, partner)

        def z_dot(c):
            if c > 0:
                @pl.when(step == 0)
                def _():
                    a_load(c).wait()
                    z = lax.dot_general(tb[...], a[pl.ds(c * CH, CH), :], DIMS_NT, preferred_element_type=F32)
                    zp[c] = z.reshape(2, 2, OWN, CH)

            @pl.when(step > 0)
            def _():
                z = jnp.dot(tb[...], at[:, c * CH:(c + 1) * CH], preferred_element_type=F32)
                zp[c] = z.reshape(2, 2, OWN, CH)

            d2d_z[c].start()

        def a_transpose(c):
            @pl.when(step == 0)
            def _():
                def block(b, carry):
                    blk = cols(b, BL)
                    at[blk, c * CH:(c + 1) * CH] = a[c * CH:(c + 1) * CH, blk].T
                    return carry

                lax.fori_loop(0, dim // BL, block, 0)

        def z_chip(c):
            d2d_z[c].wait_recv()
            zp[c, :, h] = zp[c, :, h] + zr1[c]
            ici_z[c].start()

        def r_own(c):
            ici_z[c].wait_recv()
            z = zp[c, x, h] + zr2[c]
            n = CH // 128
            labels = jnp.concatenate([y[c * n + i:c * n + i + 1, :] for i in range(n)], axis=1)
            r = labels.astype(F32) - jax.nn.sigmoid(z)
            rb[c, x, h] = r.astype(BF16)
            if c == NC - 1:
                ici_b.start()
            ici_r[c].start()
            d2d_r[c].start()

        def r_forward(c):
            ici_r[c].wait_recv()
            d2d_f[c].start()

        def gram():
            ga = lax.dot_general(tb[...], tb[0:256, :], DIMS_NT, preferred_element_type=F32)
            d2 = lax.dot_general(tb[256:384, :], tb[256:384, :], DIMS_NT, preferred_element_type=F32)
            d0, d1 = ga[0:128, 0:128], ga[128:256, 128:256]
            diag = rows3([jnp.sum(jnp.where(eye, d, 0.0), axis=0, keepdims=True) for d in (d0, d1, d2)])
            packed = jnp.concatenate(
                [ga[128:256, 0:128], ga[256:384, 0:128], ga[256:384, 128:256], jnp.where(low, d0, d1),
                 jnp.where(fold, pltpu.roll(d2[64:128], 64, 1), d2[0:64])], axis=0)
            for i in range(2):
                for j in range(2):
                    q = 2 * i + j
                    pp[i, j, 0:QR, :] = packed[QR * q:QR * (q + 1)]
                    pp[i, j, QR:QR + 8, :] = diag
            d2d_p.start()

        def gram_chip():
            d2d_p.wait_recv()
            pp[h] = pp[h] + pr1[...]
            ici_p.start()

        def kern_own():
            ici_p.wait_recv()
            pq = pp[h, x] + pr2[...]
            n_row = [pq[QR + i:QR + i + 1, :] for i in range(3)]
            n_col = [to_col(n) for n in n_row]
            pair = jnp.concatenate(
                [n_col[1] + n_row[0], n_col[2] + n_row[0], n_col[2] + n_row[1],
                 jnp.where(low, n_col[0] + n_row[0], n_col[1] + n_row[1]),
                 jnp.where(fold, n_col[2][64:128] + pltpu.roll(jnp.broadcast_to(n_row[2], (64, 128)), 64, 1),
                           n_col[2][0:64] + n_row[2])], axis=0)
            ns[...] = pair.reshape(2, 2, QR, 128)
            k = jnp.exp(-(jnp.maximum(ns[h, x] - 2.0 * pq[0:QR], 0.0) * inv_h))
            k16[h, x] = k.astype(BF16)
            ici_k.start()
            d2d_k.start()
            k32[h, x] = k
            part = unpack(k32[...].reshape(4 * QR, 128), 0.0)
            ks[h, x] = rows3([jnp.sum(part[0][j] + part[1][j] + part[2][j], axis=0, keepdims=True)
                              for j in range(3)])
            ici_s.start()
            d2d_s.start()

        def kern_forward():
            ici_k.wait_recv()
            fwd_k.start()
            ici_s.wait_recv()
            fwd_s.start()

        def kern_all():
            for cp in (d2d_k, fwd_k, d2d_s, fwd_s):
                cp.wait_recv()
            kmat = unpack(k16[...].reshape(4 * QR, 128).astype(F32), 1.0)
            total = (ks[0, 0] + ks[0, 1]) + (ks[1, 0] + ks[1, 1])
            lane = lax.broadcasted_iota(jnp.int32, (1, 128), 1)
            absent = [jnp.zeros((1, 128), F32), jnp.ones((1, 128), F32), jnp.where(lane >= 64, 1.0, 0.0)]
            for i in range(3):
                r = slice(128 * i, 128 * (i + 1))
                k0, k1, k2 = kmat[i]
                s1, s2 = pltpu.roll(k1, 64, 1), pltpu.roll(k2, 64, 1)
                first = x == 0
                ka[r, :] = jnp.where(first, jnp.concatenate([k0, jnp.where(half, k1, s2)], axis=1),
                                     jnp.concatenate([jnp.where(half, s1, s2), s2], axis=1)).astype(BF16)
                kb[r, :] = jnp.where(first, jnp.concatenate([jnp.where(half, s1, s2), jnp.where(half, s2, k2)], axis=1),
                                     jnp.concatenate([k0, jnp.where(half, k1, k2)], axis=1)).astype(BF16)
                kp[r, :] = jnp.concatenate([k0, k1], axis=1).astype(BF16)
                krow[r, :] = jnp.broadcast_to(to_col(total[i:i + 1, :] + absent[i]), (128, 128))

        def proj():
            def block(b, acc):
                blk = cols(b, BQ)
                xb = (th[:, blk] - mu[:, blk]).astype(BF16)
                return acc + lax.dot_general(xb, u[:, blk], DIMS_NT, preferred_element_type=F32)

            q = lax.fori_loop(0, dim // BQ, block, jnp.zeros((NP, 16), F32))
            qp[...] = q.T.reshape(2, 8, NP)
            d2d_q.start()

        def proj_chip():
            d2d_q.wait_recv()
            qp[h] = qp[h] + qr1[...]
            ici_q.start()

        def proj_own():
            ici_q.wait_recv()
            qf[h] = qp[h] + qr2[...]
            d2d_qg.start()

        def prior():
            d2d_qg.wait_recv()
            qb[...] = qf[...].reshape(16, NP).T.astype(BF16)

            def block(b, carry):
                blk = cols(b, BB)
                low_rank = jnp.dot(qb[...], u[:, blk], preferred_element_type=F32)
                base[:, blk] = -((th[:, blk] - mu[:, blk]) * lam[:, blk]) - low_rank
                return carry

            lax.fori_loop(0, dim // BB, block, 0)

        def pull():
            def block(b, carry):
                blk = cols(b, BK)
                t = th[:, blk]
                pulled = jnp.dot(kp[...], tb[0:256, blk], preferred_element_type=F32)
                th[:, blk] = t + c1 * (krow[:, 0:1] * t - pulled)
                return carry

            lax.fori_loop(0, dim // BK, block, 0)

        def likelihood(c, chip):
            rows = chip_rows(chip)

            def block(b, carry):
                blk = cols(b, BR)
                ra = jnp.dot(rb[c, chip].reshape(2 * OWN, CH), a[pl.ds(c * CH, CH), blk], preferred_element_type=F32)
                base[rows, blk] = base[rows, blk] + beta * ra
                return carry

            lax.fori_loop(0, dim // BR, block, 0)

        def likelihood_near(c):
            d2d_r[c].wait_recv()
            likelihood(c, x)

        def likelihood_far(c):
            d2d_f[c].wait_recv()
            likelihood(c, ox)

        def update_near(c):
            d2d_r[c].wait_recv()

            def block(b, carry):
                blk = cols(b, BU)
                th[:, blk] = drive(beta, c2, two_h, th, base, a, tb, rb, c, x, ka, 256, blk)
                return carry

            lax.fori_loop(0, dim // BU, block, 0)

        def update_far(c):
            ici_r[c].wait_recv()
            ici_b.wait_recv()

            def block(b, carry):
                blk = cols(b, BU)
                t = drive(beta, c2, two_h, th, base, a, tb, rb, c, ox, kb, 320, blk)
                th[:, blk] = t
                tb[:, blk] = t.astype(BF16)
                return carry

            @pl.when(step < NUM_STEPS - 1)
            def _():
                lax.fori_loop(0, dim // BU, block, 0)

        z_dot(0)
        gram()
        z_chip(0)
        z_dot(1)
        proj()
        gram_chip()
        proj_chip()
        z_chip(1)
        z_dot(2)
        a_transpose(0)
        kern_own()
        z_chip(2)
        proj_own()
        a_transpose(1)
        r_own(0)
        prior()
        r_own(1)
        a_transpose(2)
        likelihood_near(0)
        kern_forward()
        likelihood_near(1)
        kern_all()
        r_own(2)
        pull()
        r_forward(0)
        update_near(2)
        r_forward(1)
        likelihood_far(0)
        likelihood_far(1)
        update_far(2)

        for cp in d2d_z + ici_z + ici_r + d2d_r + d2d_f + [
                ici_b, d2d_p, ici_p, ici_k, d2d_k, fwd_k, ici_s, d2d_s, fwd_s, d2d_q, ici_q, d2d_qg]:
            cp.wait_send()
        return carry

    lax.fori_loop(0, NUM_STEPS, step_body, 0)


def solution(mesh):
    feat_size = mesh.shape["feat"]

    def local_run(particles, prec_diag, low_factor, prior_mean, data_mat, labels):
        n_part, dim_local = particles.shape
        dim_full = dim_local * feat_size
        m_rows = data_mat.shape[0]
        band_width = 2.0 * dim_full
        step_size = dim_full / 4.0
        beta = 2.0 / math.sqrt(m_rows * dim_full)
        c1 = step_size * (2.0 / band_width) / n_part
        c2 = step_size / n_part
        nb = dim_local // BL
        vm = pltpu.VMEM
        scratch = [
            vm((1, dim_local), F32),
            vm((1, dim_local), F32),
            vm((16, dim_local), BF16),
            vm((m_rows // 128, 128), jnp.int32),
            vm((dim_local, MD), BF16),
            vm((NC, 2, 2, OWN, CH), F32),
            vm((NC, 2, OWN, CH), F32),
            vm((NC, OWN, CH), F32),
            vm((2, 2, QR + 8, 128), F32),
            vm((2, QR + 8, 128), F32),
            vm((QR + 8, 128), F32),
            vm((2, 2, QR, 128), F32),
            vm((2, 2, QR, 128), F32),
            vm((2, 2, QR, 128), BF16),
            vm((2, 2, 8, 128), F32),
            vm((2, 8, NP), F32),
            vm((8, NP), F32),
            vm((8, NP), F32),
            vm((2, 8, NP), F32),
            vm((NP, 256), BF16),
            vm((NP, 256), BF16),
            vm((NP, 128), F32),
            vm((NP, 16), BF16),
            pltpu.SemaphoreType.DMA((N_SEM,)),
            pltpu.SemaphoreType.DMA((N_SEM,)),
            pltpu.SemaphoreType.DMA((nb + NC + 4 + NF,)),
        ]
        hspec = pl.BlockSpec(memory_space=pltpu.HBM)
        vspec = pl.BlockSpec(memory_space=pltpu.VMEM)
        kept = pl.pallas_call(
            functools.partial(kernel, beta, c1, c2, 2.0 / band_width, 1.0 / band_width),
            out_shape=[
                vm((n_part, dim_local), F32),
                vm((n_part, dim_local), F32),
                vm((m_rows, dim_local), BF16),
                vm((n_part, dim_local), BF16),
                vm((NC, 2, 2, OWN, CH), BF16),
                vm((n_part, 256), BF16),
            ],
            in_specs=[hspec] * 6,
            out_specs=[vspec] * 6,
            scratch_shapes=scratch,
            compiler_params=pltpu.CompilerParams(
                collective_id=0, has_side_effects=True, vmem_limit_bytes=VMEM_STEPS),
            name="svgd",
        )(particles, prec_diag.reshape(1, dim_local), prior_mean.reshape(1, dim_local), low_factor.T,
          data_mat, labels.reshape(m_rows // 128, 128))
        return pl.pallas_call(
            functools.partial(last_kernel, beta, c2, 2.0 / band_width),
            out_shape=jax.ShapeDtypeStruct((n_part, dim_local), F32),
            in_specs=[vspec] * 6,
            out_specs=hspec,
            scratch_shapes=[vm((n_part, dim_local), F32), pltpu.SemaphoreType.DMA((dim_local // BO,))],
            compiler_params=pltpu.CompilerParams(vmem_limit_bytes=12 * 1024 * 1024),
            name="svgd_last",
        )(*kept)

    return jax.shard_map(
        local_run,
        mesh=mesh,
        in_specs=(P("ens", "feat"), P(("ens", "feat")), P(("ens", "feat"), None),
                  P(("ens", "feat")), P("ens", "feat"), P("ens")),
        out_specs=P("ens", "feat"),
        check_vma=False,
    )
```

```python
import functools
import math

import jax
import jax.numpy as jnp
from jax import lax
from jax.experimental import pallas as pl
from jax.experimental.pallas import tpu as pltpu
from jax.sharding import PartitionSpec as P

NUM_STEPS = 3
DIMS_NT = (((1,), (1,)), ((), ()))
MESH = pl.DeviceIdType.MESH
F32 = jnp.float32
BF16 = jnp.bfloat16

NP = 384
MD = 768
CH = 256
NC = MD // CH
OWN = NP // 4
QR = 144
BL = 512
BQ = 4096
BB = 2048
BK = 4096
BR = 4096
BU = 4096
NF = 4
BO = 1024

VMEM_STEPS = 43_000_000

D2D_Z, ICI_Z, ICI_R, D2D_R, D2D_F = 0, NC, 2 * NC, 3 * NC, 4 * NC
(D2D_P, ICI_P, ICI_K, D2D_K, FWD_K, ICI_S, D2D_S, FWD_S,
 D2D_Q, ICI_Q, D2D_QG) = range(5 * NC, 5 * NC + 11)
N_SEM = 5 * NC + 11


def chip_rows(chip):
    return pl.ds(pl.multiple_of(2 * OWN * chip, 2 * OWN), 2 * OWN)


def drive(beta, c2, two_h, th, base, a, tb, rb, c, chip, kx, j0, blk):
    ra = jnp.dot(rb[c, chip].reshape(2 * OWN, CH), a[pl.ds(c * CH, CH), blk], preferred_element_type=F32)
    s = (base[chip_rows(chip), blk] + beta * ra).astype(BF16)
    rhs = jnp.concatenate([s, tb[j0:j0 + 64, blk] * (-two_h)], axis=0)
    return th[:, blk] + c2 * jnp.dot(kx[...], rhs, preferred_element_type=F32)


def last_kernel(beta, c2, two_h, th, base, a, tb, rb, kb, out_hbm, out, sems):
    ox = 1 - lax.div(lax.axis_index("feat"), 2)
    copies = []
    for b in range(th.shape[1] // BO):
        blk = pl.ds(b * BO, BO)
        out[:, blk] = drive(beta, c2, two_h, th, base, a, tb, rb, NC - 1, ox, kb, 320, blk)
        copies.append(pltpu.make_async_copy(out.at[:, blk], out_hbm.at[:, blk], sems.at[b]))
        copies[-1].start()
    for cp in copies:
        cp.wait()


def kernel(beta, c1, c2, two_h, inv_h, th_hbm, lam_hbm, mu_hbm, u_hbm, a_hbm, y_hbm, th, base, a, tb, rb, kb,
           lam, mu, u, y, at, zp, zr1, zr2, pp, pr1, pr2, ns, k32, k16, ks, qp, qr1, qr2, qf,
           ka, kp, krow, qb, ss, rs, ls):
    dim = th.shape[1]
    nb = dim // BL
    me = lax.axis_index("feat")
    x, core = lax.div(me, 2), lax.rem(me, 2)
    ox, oc = 1 - x, 1 - core
    partner, cross, peer = x * 2 + oc, ox * 2 + oc, ox * 2 + core
    h = lax.rem(x + core, 2)
    oh = 1 - h

    def remote(src, dst, slot, dev):
        return pltpu.make_async_remote_copy(
            src_ref=src, dst_ref=dst, send_sem=ss.at[slot], recv_sem=rs.at[slot],
            device_id={"feat": dev}, device_id_type=MESH)

    def cols(b, size):
        return pl.ds(pl.multiple_of(b * size, size), size)

    def th_load(b):
        return pltpu.make_async_copy(th_hbm.at[:, cols(b, BL)], th.at[:, cols(b, BL)], ls.at[b])

    def a_load(c):
        return pltpu.make_async_copy(a_hbm.at[pl.ds(c * CH, CH)], a.at[pl.ds(c * CH, CH)], ls.at[nb + c])

    small = [pltpu.make_async_copy(src, dst, ls.at[nb + NC + i])
             for i, (src, dst) in enumerate([(lam_hbm, lam), (mu_hbm, mu), (u_hbm, u), (y_hbm, y)])]
    def a_first(i):
        part = pl.ds(i * (dim // NF), dim // NF)
        return pltpu.make_async_copy(a_hbm.at[pl.ds(0, CH), part], a.at[pl.ds(0, CH), part], ls.at[nb + NC + 4 + i])

    for i in range(NF):
        for b in range(i * nb // NF, (i + 1) * nb // NF):
            th_load(b).start()
        a_first(i).start()
    for cp in small:
        cp.start()

    barrier = pltpu.get_barrier_semaphore()
    for dev in (partner, cross, peer):
        pl.semaphore_signal(barrier, inc=1, device_id={"feat": dev}, device_id_type=MESH)
    pl.semaphore_wait(barrier, 3)

    k32[...] = jnp.zeros_like(k32)

    def conv(b, carry):
        th_load(b).wait()
        tb[:, cols(b, BL)] = th[:, cols(b, BL)].astype(BF16)
        return carry

    for i in range(NF):
        part = slice(i * (dim // NF), (i + 1) * (dim // NF))
        lax.fori_loop(i * nb // NF, (i + 1) * nb // NF, conv, 0)
        a_first(i).wait()
        if i == NF - 1:
            for c in range(1, NC):
                a_load(c).start()
        z = lax.dot_general(tb[:, part], a[0:CH, part], DIMS_NT, preferred_element_type=F32).reshape(2, 2, OWN, CH)
        zp[0] = z if i == 0 else zp[0] + z
    for cp in small:
        cp.wait()

    ri = lax.broadcasted_iota(jnp.int32, (128, 128), 0)
    ci = lax.broadcasted_iota(jnp.int32, (128, 128), 1)
    eye, low, half = ri == ci, ri >= ci, ci < 64
    r64 = lax.broadcasted_iota(jnp.int32, (64, 128), 0)
    c64 = lax.broadcasted_iota(jnp.int32, (64, 128), 1)
    fold = (c64 < 64) & (r64 < c64)
    straight = ((ri < 64) & ((ci >= 64) | low)) | ((ri >= 64) & (ci > ri))
    r8 = lax.broadcasted_iota(jnp.int32, (8, 128), 0)

    def rows3(v):
        return jnp.where(r8 == 0, v[0], jnp.where(r8 == 1, v[1], jnp.where(r8 == 2, v[2], 0.0)))

    def to_col(row):
        return jnp.sum(jnp.where(eye, row, 0.0), axis=1, keepdims=True)

    def unpack(p, one):
        m10, m20, m21, mix, m2 = p[0:128], p[128:256], p[256:384], p[384:512], p[512:576]
        mix_t = mix.T
        d0 = jnp.where(low, mix, mix_t)
        d1 = jnp.where(ri < ci, mix, jnp.where(eye, one, mix_t))
        f = jnp.concatenate([m2, pltpu.roll(m2, 64, 1)], axis=0)
        d2 = jnp.where(straight, f, jnp.where(eye & (ri >= 64), one, f.T))
        return [[d0, m10.T, m20.T], [m10, d1, m21.T], [m20, m21, d2]]

    def step_body(step, carry):
        d2d_z = [remote(zp.at[c, :, oh], zr1.at[c], D2D_Z + c, partner) for c in range(NC)]
        ici_z = [remote(zp.at[c, ox, h], zr2.at[c], ICI_Z + c, cross) for c in range(NC)]
        ici_r = [remote(rb.at[c, x, h], rb.at[c, x, h], ICI_R + c, cross) for c in range(NC)]
        d2d_r = [remote(rb.at[c, x, h], rb.at[c, x, h], D2D_R + c, partner) for c in range(NC)]
        d2d_f = [remote(rb.at[c, ox, h], rb.at[c, ox, h], D2D_F + c, partner) for c in range(NC - 1)]
        ici_b = remote(rb.at[NC - 1, x, h], rb.at[NC - 1, x, h], D2D_F + NC - 1, peer)
        d2d_p = remote(pp.at[oh], pr1, D2D_P, partner)
        ici_p = remote(pp.at[h, ox], pr2, ICI_P, cross)
        ici_k = remote(k16.at[h, x], k16.at[h, x], ICI_K, cross)
        d2d_k = remote(k16.at[h, x], k16.at[h, x], D2D_K, partner)
        fwd_k = remote(k16.at[h, ox], k16.at[h, ox], FWD_K, partner)
        ici_s = remote(ks.at[h, x], ks.at[h, x], ICI_S, cross)
        d2d_s = remote(ks.at[h, x], ks.at[h, x], D2D_S, partner)
        fwd_s = remote(ks.at[h, ox], ks.at[h, ox], FWD_S, partner)
        d2d_q = remote(qp.at[oh], qr1, D2D_Q, partner)
        ici_q = remote(qp.at[h], qr2, ICI_Q, cross)
        d2d_qg = remote(qf.at[h], qf.at[h], D2D_QG, partner)

        def z_dot(c):
            if c > 0:
                @pl.when(step == 0)
                def _():
                    a_load(c).wait()
                    z = lax.dot_general(tb[...], a[pl.ds(c * CH, CH), :], DIMS_NT, preferred_element_type=F32)
                    zp[c] = z.reshape(2, 2, OWN, CH)

            @pl.when(step > 0)
            def _():
                z = jnp.dot(tb[...], at[:, c * CH:(c + 1) * CH], preferred_element_type=F32)
                zp[c] = z.reshape(2, 2, OWN, CH)

            d2d_z[c].start()

        def a_transpose(c):
            @pl.when(step == 0)
            def _():
                def block(b, carry):
                    blk = cols(b, BL)
                    at[blk, c * CH:(c + 1) * CH] = a[c * CH:(c + 1) * CH, blk].T
                    return carry

                lax.fori_loop(0, dim // BL, block, 0)

        def z_chip(c):
            d2d_z[c].wait_recv()
            zp[c, :, h] = zp[c, :, h] + zr1[c]
            ici_z[c].start()

        def r_own(c):
            ici_z[c].wait_recv()
            z = zp[c, x, h] + zr2[c]
            n = CH // 128
            labels = jnp.concatenate([y[c * n + i:c * n + i + 1, :] for i in range(n)], axis=1)
            r = labels.astype(F32) - jax.nn.sigmoid(z)
            rb[c, x, h] = r.astype(BF16)
            ici_r[c].start()
            if c == NC - 1:
                ici_b.start()
            d2d_r[c].start()

        def r_forward(c):
            ici_r[c].wait_recv()
            d2d_f[c].start()

        def gram():
            ga = lax.dot_general(tb[...], tb[0:256, :], DIMS_NT, preferred_element_type=F32)
            d2 = lax.dot_general(tb[256:384, :], tb[256:384, :], DIMS_NT, preferred_element_type=F32)
            d0, d1 = ga[0:128, 0:128], ga[128:256, 128:256]
            diag = rows3([jnp.sum(jnp.where(eye, d, 0.0), axis=0, keepdims=True) for d in (d0, d1, d2)])
            packed = jnp.concatenate(
                [ga[128:256, 0:128], ga[256:384, 0:128], ga[256:384, 128:256], jnp.where(low, d0, d1),
                 jnp.where(fold, pltpu.roll(d2[64:128], 64, 1), d2[0:64])], axis=0)
            for i in range(2):
                for j in range(2):
                    q = 2 * i + j
                    pp[i, j, 0:QR, :] = packed[QR * q:QR * (q + 1)]
                    pp[i, j, QR:QR + 8, :] = diag
            d2d_p.start()

        def gram_chip():
            d2d_p.wait_recv()
            pp[h] = pp[h] + pr1[...]
            ici_p.start()

        def kern_own():
            ici_p.wait_recv()
            pq = pp[h, x] + pr2[...]
            n_row = [pq[QR + i:QR + i + 1, :] for i in range(3)]
            n_col = [to_col(n) for n in n_row]
            pair = jnp.concatenate(
                [n_col[1] + n_row[0], n_col[2] + n_row[0], n_col[2] + n_row[1],
                 jnp.where(low, n_col[0] + n_row[0], n_col[1] + n_row[1]),
                 jnp.where(fold, n_col[2][64:128] + pltpu.roll(jnp.broadcast_to(n_row[2], (64, 128)), 64, 1),
                           n_col[2][0:64] + n_row[2])], axis=0)
            ns[...] = pair.reshape(2, 2, QR, 128)
            k = jnp.exp(-(jnp.maximum(ns[h, x] - 2.0 * pq[0:QR], 0.0) * inv_h))
            k16[h, x] = k.astype(BF16)
            ici_k.start()
            d2d_k.start()
            k32[h, x] = k
            part = unpack(k32[...].reshape(4 * QR, 128), 0.0)
            ks[h, x] = rows3([jnp.sum(part[0][j] + part[1][j] + part[2][j], axis=0, keepdims=True)
                              for j in range(3)])
            ici_s.start()
            d2d_s.start()

        def kern_forward():
            ici_k.wait_recv()
            fwd_k.start()
            ici_s.wait_recv()
            fwd_s.start()

        def kern_all():
            for cp in (d2d_k, fwd_k, d2d_s, fwd_s):
                cp.wait_recv()
            kmat = unpack(k16[...].reshape(4 * QR, 128).astype(F32), 1.0)
            total = (ks[0, 0] + ks[0, 1]) + (ks[1, 0] + ks[1, 1])
            lane = lax.broadcasted_iota(jnp.int32, (1, 128), 1)
            absent = [jnp.zeros((1, 128), F32), jnp.ones((1, 128), F32), jnp.where(lane >= 64, 1.0, 0.0)]
            for i in range(3):
                r = slice(128 * i, 128 * (i + 1))
                k0, k1, k2 = kmat[i]
                s1, s2 = pltpu.roll(k1, 64, 1), pltpu.roll(k2, 64, 1)
                first = x == 0
                ka[r, :] = jnp.where(first, jnp.concatenate([k0, jnp.where(half, k1, s2)], axis=1),
                                     jnp.concatenate([jnp.where(half, s1, s2), s2], axis=1)).astype(BF16)
                kb[r, :] = jnp.where(first, jnp.concatenate([jnp.where(half, s1, s2), jnp.where(half, s2, k2)], axis=1),
                                     jnp.concatenate([k0, jnp.where(half, k1, k2)], axis=1)).astype(BF16)
                kp[r, :] = jnp.concatenate([k0, k1], axis=1).astype(BF16)
                krow[r, :] = jnp.broadcast_to(to_col(total[i:i + 1, :] + absent[i]), (128, 128))

        def proj():
            def block(b, acc):
                blk = cols(b, BQ)
                xb = (th[:, blk] - mu[:, blk]).astype(BF16)
                return acc + lax.dot_general(xb, u[:, blk], DIMS_NT, preferred_element_type=F32)

            q = lax.fori_loop(0, dim // BQ, block, jnp.zeros((NP, 16), F32))
            qp[...] = q.T.reshape(2, 8, NP)
            d2d_q.start()

        def proj_chip():
            d2d_q.wait_recv()
            qp[h] = qp[h] + qr1[...]
            ici_q.start()

        def proj_own():
            ici_q.wait_recv()
            qf[h] = qp[h] + qr2[...]
            d2d_qg.start()

        def prior():
            d2d_qg.wait_recv()
            qb[...] = qf[...].reshape(16, NP).T.astype(BF16)

            def block(b, carry):
                blk = cols(b, BB)
                low_rank = jnp.dot(qb[...], u[:, blk], preferred_element_type=F32)
                base[:, blk] = -((th[:, blk] - mu[:, blk]) * lam[:, blk]) - low_rank
                return carry

            lax.fori_loop(0, dim // BB, block, 0)

        def pull():
            def block(b, carry):
                blk = cols(b, BK)
                t = th[:, blk]
                pulled = jnp.dot(kp[...], tb[0:256, blk], preferred_element_type=F32)
                th[:, blk] = t + c1 * (krow[:, 0:1] * t - pulled)
                return carry

            lax.fori_loop(0, dim // BK, block, 0)

        def likelihood(c, chip):
            rows = chip_rows(chip)

            def block(b, carry):
                blk = cols(b, BR)
                ra = jnp.dot(rb[c, chip].reshape(2 * OWN, CH), a[pl.ds(c * CH, CH), blk], preferred_element_type=F32)
                base[rows, blk] = base[rows, blk] + beta * ra
                return carry

            lax.fori_loop(0, dim // BR, block, 0)

        def likelihood_near(c):
            d2d_r[c].wait_recv()
            likelihood(c, x)

        def likelihood_far(c):
            d2d_f[c].wait_recv()
            likelihood(c, ox)

        def update_near(c):
            d2d_r[c].wait_recv()

            def block(b, carry):
                blk = cols(b, BU)
                th[:, blk] = drive(beta, c2, two_h, th, base, a, tb, rb, c, x, ka, 256, blk)
                return carry

            lax.fori_loop(0, dim // BU, block, 0)

        def update_far(c):
            ici_r[c].wait_recv()
            ici_b.wait_recv()

            def block(b, carry):
                blk = cols(b, BU)
                t = drive(beta, c2, two_h, th, base, a, tb, rb, c, ox, kb, 320, blk)
                th[:, blk] = t
                tb[:, blk] = t.astype(BF16)
                return carry

            @pl.when(step < NUM_STEPS - 1)
            def _():
                lax.fori_loop(0, dim // BU, block, 0)

        z_dot(0)
        gram()
        z_chip(0)
        z_dot(1)
        proj()
        gram_chip()
        proj_chip()
        z_chip(1)
        z_dot(2)
        a_transpose(0)
        kern_own()
        z_chip(2)
        proj_own()
        a_transpose(1)
        r_own(0)
        prior()
        r_own(1)
        a_transpose(2)
        likelihood_near(0)
        kern_forward()
        likelihood_near(1)
        kern_all()
        r_own(2)
        pull()
        r_forward(0)
        update_near(2)
        r_forward(1)
        likelihood_far(0)
        likelihood_far(1)
        update_far(2)

        for cp in d2d_z + ici_z + ici_r + d2d_r + d2d_f + [
                ici_b, d2d_p, ici_p, ici_k, d2d_k, fwd_k, ici_s, d2d_s, fwd_s, d2d_q, ici_q, d2d_qg]:
            cp.wait_send()
        return carry

    lax.fori_loop(0, NUM_STEPS, step_body, 0)


def solution(mesh):
    feat_size = mesh.shape["feat"]

    def local_run(particles, prec_diag, low_factor, prior_mean, data_mat, labels):
        n_part, dim_local = particles.shape
        dim_full = dim_local * feat_size
        m_rows = data_mat.shape[0]
        band_width = 2.0 * dim_full
        step_size = dim_full / 4.0
        beta = 2.0 / math.sqrt(m_rows * dim_full)
        c1 = step_size * (2.0 / band_width) / n_part
        c2 = step_size / n_part
        nb = dim_local // BL
        vm = pltpu.VMEM
        scratch = [
            vm((1, dim_local), F32),
            vm((1, dim_local), F32),
            vm((16, dim_local), BF16),
            vm((m_rows // 128, 128), jnp.int32),
            vm((dim_local, MD), BF16),
            vm((NC, 2, 2, OWN, CH), F32),
            vm((NC, 2, OWN, CH), F32),
            vm((NC, OWN, CH), F32),
            vm((2, 2, QR + 8, 128), F32),
            vm((2, QR + 8, 128), F32),
            vm((QR + 8, 128), F32),
            vm((2, 2, QR, 128), F32),
            vm((2, 2, QR, 128), F32),
            vm((2, 2, QR, 128), BF16),
            vm((2, 2, 8, 128), F32),
            vm((2, 8, NP), F32),
            vm((8, NP), F32),
            vm((8, NP), F32),
            vm((2, 8, NP), F32),
            vm((NP, 256), BF16),
            vm((NP, 256), BF16),
            vm((NP, 128), F32),
            vm((NP, 16), BF16),
            pltpu.SemaphoreType.DMA((N_SEM,)),
            pltpu.SemaphoreType.DMA((N_SEM,)),
            pltpu.SemaphoreType.DMA((nb + NC + 4 + NF,)),
        ]
        hspec = pl.BlockSpec(memory_space=pltpu.HBM)
        vspec = pl.BlockSpec(memory_space=pltpu.VMEM)
        kept = pl.pallas_call(
            functools.partial(kernel, beta, c1, c2, 2.0 / band_width, 1.0 / band_width),
            out_shape=[
                vm((n_part, dim_local), F32),
                vm((n_part, dim_local), F32),
                vm((m_rows, dim_local), BF16),
                vm((n_part, dim_local), BF16),
                vm((NC, 2, 2, OWN, CH), BF16),
                vm((n_part, 256), BF16),
            ],
            in_specs=[hspec] * 6,
            out_specs=[vspec] * 6,
            scratch_shapes=scratch,
            compiler_params=pltpu.CompilerParams(
                collective_id=0, has_side_effects=True, vmem_limit_bytes=VMEM_STEPS),
            name="svgd",
        )(particles, prec_diag.reshape(1, dim_local), prior_mean.reshape(1, dim_local), low_factor.T,
          data_mat, labels.reshape(m_rows // 128, 128))
        return pl.pallas_call(
            functools.partial(last_kernel, beta, c2, 2.0 / band_width),
            out_shape=jax.ShapeDtypeStruct((n_part, dim_local), F32),
            in_specs=[vspec] * 6,
            out_specs=hspec,
            scratch_shapes=[vm((n_part, dim_local), F32), pltpu.SemaphoreType.DMA((dim_local // BO,))],
            compiler_params=pltpu.CompilerParams(vmem_limit_bytes=12 * 1024 * 1024),
            name="svgd_last",
        )(*kept)

    return jax.shard_map(
        local_run,
        mesh=mesh,
        in_specs=(P("ens", "feat"), P(("ens", "feat")), P(("ens", "feat"), None),
                  P(("ens", "feat")), P("ens", "feat"), P("ens")),
        out_specs=P("ens", "feat"),
        check_vma=False,
    )
```
